16 devices in a mesh: t: 4 (over z, y), v: 4 (over x, core).
Axes of the slice: x: 2, y: 2, z: 2, core: 2. Of those that a mesh axis runs over, the one named last changes fastest.
Arguments:
- hidden_in: bfloat16 [1024, 2304], replicated
- seq_lens: int32 [1024], replicated
- target: int32 [1024], replicated
- g_attn_pre: bfloat16 [2304], replicated
- w_q: bfloat16 [2304, 2048], P(None, 't')
- w_k: bfloat16 [2304, 1024], P(None, 't')
- w_v: bfloat16 [2304, 1024], P(None, 't')
- w_o: bfloat16 [2048, 2304], P('t')
- g_attn_post: bfloat16 [2304], replicated
- g_mlp_pre: bfloat16 [2304], replicated
- w_gate: bfloat16 [2304, 9216], P(None, 't')
- w_up: bfloat16 [2304, 9216], P(None, 't')
- w_down: bfloat16 [9216, 2304], P('t')
- g_mlp_post: bfloat16 [2304], replicated
- g_final: bfloat16 [2304], replicated
- k_cache: bfloat16 [1024, 32, 4, 256], P(None, None, 't')
- v_cache: bfloat16 [1024, 32, 4, 256], P(None, None, 't')
- embed_table: bfloat16 [256000, 2304], P(('v', 't'))
Outputs:
- output 1: float32 [1024], replicated
- output 2: bfloat16 [1024, 2304], replicated
All inputs are finite; a program needn't handle non-finite values.
Results may differ from the reference program's by a relative error of at most 0.00785292.
Values sent between devices are 32-bit elements.
A program may use at most 1 GiB of HBM per device.

```python
import jax
import jax.numpy as jnp
from jax import lax

D = 2304
HEADS = 8
KV_HEADS = 4
HEAD = 256
FF = 9216
VOCAB = 256000
TOKENS = 1024
CTX = 32

ATTN_CAP = 50.0
FINAL_CAP = 30.0
NORM_EPS = 1e-6
ROPE_BASE = 10000.0


def rms_norm(values, gain_vec):
    x_f32 = values.astype(jnp.float32)
    scaled = x_f32 * lax.rsqrt(jnp.mean(x_f32 * x_f32, axis=-1, keepdims=True) + NORM_EPS)
    return scaled * (1.0 + gain_vec.astype(jnp.float32))


def rotary(values, positions):
    half_dim = values.shape[-1] // 2
    inv_freq = ROPE_BASE ** (-2.0 * jnp.arange(half_dim, dtype=jnp.float32) / values.shape[-1])
    angles = positions.astype(jnp.float32)[:, None] * inv_freq[None, :]
    angles = angles.reshape((values.shape[0],) + (1,) * (values.ndim - 2) + (half_dim,))
    cos_t = jnp.cos(angles)
    sin_t = jnp.sin(angles)
    x_low = values[..., :half_dim]
    x_high = values[..., half_dim:]
    return jnp.concatenate([x_low * cos_t - x_high * sin_t, x_high * cos_t + x_low * sin_t], axis=-1)


def setup_inputs(seed: int = 0) -> dict:
    keys = jax.random.split(jax.random.key(seed), 20)

    def normal_draw(sub_key, dims, scale_by):
        return (jax.random.normal(sub_key, dims, jnp.float32) * scale_by).astype(jnp.bfloat16)

    int_keys = jax.random.split(keys[19], 4)
    token_ids = jnp.arange(TOKENS)
    seq_lens = jax.random.randint(int_keys[0], (TOKENS,), 1, CTX + 1)
    picked = jax.random.permutation(int_keys[1], TOKENS)
    seq_lens = jnp.where(token_ids == picked[0], CTX, seq_lens)
    seq_lens = jnp.where(token_ids == picked[1], 1, seq_lens).astype(jnp.int32)
    stride = VOCAB // TOKENS
    target = token_ids * stride + jax.random.randint(int_keys[2], (TOKENS,), 0, stride)
    target = jax.random.permutation(int_keys[3], target).astype(jnp.int32)
    d_scale = D ** -0.5
    return {
        'hidden_in': normal_draw(keys[0], (TOKENS, D), 1.0),
        'seq_lens': seq_lens,
        'target': target,
        'g_attn_pre': normal_draw(keys[1], (D,), 0.4),
        'w_q': normal_draw(keys[2], (D, HEADS * HEAD), 4.0 * d_scale),
        'w_k': normal_draw(keys[3], (D, KV_HEADS * HEAD), 4.0 * d_scale),
        'w_v': normal_draw(keys[4], (D, KV_HEADS * HEAD), d_scale),
        'w_o': normal_draw(keys[5], (HEADS * HEAD, D), (HEADS * HEAD) ** -0.5),
        'g_attn_post': normal_draw(keys[6], (D,), 0.4),
        'g_mlp_pre': normal_draw(keys[7], (D,), 0.4),
        'w_gate': normal_draw(keys[8], (D, FF), d_scale),
        'w_up': normal_draw(keys[9], (D, FF), d_scale),
        'w_down': normal_draw(keys[10], (FF, D), FF ** -0.5),
        'g_mlp_post': normal_draw(keys[11], (D,), 0.4),
        'g_final': normal_draw(keys[12], (D,), 0.4),
        'k_cache': normal_draw(keys[13], (TOKENS, CTX, KV_HEADS, HEAD), 4.0),
        'v_cache': normal_draw(keys[14], (TOKENS, CTX, KV_HEADS, HEAD), 1.0),
        'embed_table': normal_draw(keys[15], (VOCAB, D), 25.0 * d_scale),
    }


def reference(hidden_in, seq_lens, target, g_attn_pre, w_q, w_k, w_v, w_o, g_attn_post, g_mlp_pre, w_gate, w_up, w_down, g_mlp_post, g_final, k_cache, v_cache, embed_table):
    group_size = HEADS // KV_HEADS
    score_scale = HEAD ** -0.5
    normed = rms_norm(hidden_in, g_attn_pre).astype(jnp.bfloat16)
    q_rot = rotary(jnp.dot(normed, w_q, preferred_element_type=jnp.float32).reshape(TOKENS, KV_HEADS, group_size, HEAD), seq_lens).astype(jnp.bfloat16)
    k_rot = rotary(jnp.dot(normed, w_k, preferred_element_type=jnp.float32).reshape(TOKENS, KV_HEADS, HEAD), seq_lens).astype(jnp.bfloat16)
    v_new = jnp.dot(normed, w_v, preferred_element_type=jnp.float32).astype(jnp.bfloat16).reshape(TOKENS, KV_HEADS, HEAD)

    def attend(operands):
        q_tok, k_tok, v_tok, keys_tok, vals_tok, len_tok = operands
        q_f32 = q_tok.astype(jnp.float32)
        s_cache = jnp.einsum('kgd,tkd->kgt', q_f32, keys_tok.astype(jnp.float32)) * score_scale
        s_new = jnp.einsum('kgd,kd->kg', q_f32, k_tok.astype(jnp.float32)) * score_scale
        s_cache = ATTN_CAP * jnp.tanh(s_cache / ATTN_CAP)
        s_new = ATTN_CAP * jnp.tanh(s_new / ATTN_CAP)
        s_cache = jnp.where(jnp.arange(CTX) < len_tok, s_cache, -1e30)
        row_max = jnp.maximum(jnp.max(s_cache, axis=-1), s_new)
        p_cache = jnp.exp(s_cache - row_max[..., None])
        p_new = jnp.exp(s_new - row_max)
        denominator = jnp.sum(p_cache, axis=-1) + p_new
        weighted = jnp.einsum('kgt,tkd->kgd', p_cache.astype(jnp.bfloat16).astype(jnp.float32), vals_tok.astype(jnp.float32))
        weighted = weighted + p_new.astype(jnp.bfloat16).astype(jnp.float32)[..., None] * v_tok.astype(jnp.float32)[:, None, :]
        return (weighted / denominator[..., None]).astype(jnp.bfloat16)

    attn_vec = lax.map(attend, (q_rot, k_rot, v_new, k_cache, v_cache, seq_lens))
    attn_out = jnp.dot(attn_vec.reshape(TOKENS, HEADS * HEAD), w_o, preferred_element_type=jnp.float32)
    hidden_mid = (hidden_in.astype(jnp.float32) + rms_norm(attn_out, g_attn_post)).astype(jnp.bfloat16)
    mlp_in = rms_norm(hidden_mid, g_mlp_pre).astype(jnp.bfloat16)
    gate_proj = jnp.dot(mlp_in, w_gate, preferred_element_type=jnp.float32)
    up_proj = jnp.dot(mlp_in, w_up, preferred_element_type=jnp.float32)
    activated = (jax.nn.gelu(gate_proj, approximate=True) * up_proj).astype(jnp.bfloat16)
    mlp_out = jnp.dot(activated, w_down, preferred_element_type=jnp.float32)
    hidden_out = (hidden_mid.astype(jnp.float32) + rms_norm(mlp_out, g_mlp_post)).astype(jnp.bfloat16)
    final_h = rms_norm(hidden_out, g_final).astype(jnp.bfloat16)

    blocks = 16
    block_rows = VOCAB // blocks
    table_blocks = embed_table.reshape(blocks, block_rows, D)
    starts = jnp.arange(blocks) * block_rows

    def block_stats(operands):
        table_block, start_row = operands
        logits = jnp.dot(final_h, table_block.T, preferred_element_type=jnp.float32)
        capped = FINAL_CAP * jnp.tanh(logits / FINAL_CAP)
        block_max = jnp.max(capped, axis=1)
        block_sum = jnp.sum(jnp.exp(capped - block_max[:, None]), axis=1)
        hit_mask = (start_row + jnp.arange(block_rows))[None, :] == target[:, None]
        block_tgt = jnp.sum(jnp.where(hit_mask, capped, 0.0), axis=1)
        return block_max, block_sum, block_tgt

    all_max, all_sum, all_tgt = lax.map(block_stats, (table_blocks, starts))
    glob_max = jnp.max(all_max, axis=0)
    log_norm = glob_max + jnp.log(jnp.sum(all_sum * jnp.exp(all_max - glob_max[None, :]), axis=0))
    logprob = jnp.sum(all_tgt, axis=0) - log_norm
    return logprob, hidden_out
```

```python
import functools

import jax
import jax.numpy as jnp
from jax import lax
from jax.experimental import pallas as pl
from jax.experimental.pallas import tpu as pltpu
from jax.sharding import PartitionSpec as P

ATTN_CAP = 50.0
FINAL_CAP = 30.0
NORM_EPS = 1e-6
ROPE_BASE = 10000.0
MESH = pl.DeviceIdType.MESH
F32 = jnp.float32
BF16 = jnp.bfloat16

CHUNKS = 2
E_ROWS = 800
E_SLOTS = 4


def flip_t(t, mask):
    if mask == 0:
        return t
    if mask == 1:
        return t + 1 - 2 * (t % 2)
    if mask == 2:
        return (t + 2) % 4
    return 3 - t


def flip_v(v, mask):
    return flip_t(v, mask)


def rms(values, gain):
    return values * lax.rsqrt(jnp.mean(values * values, axis=-1, keepdims=True) + NORM_EPS) * gain


def layer_kernel(x_hbm, seq_ref, cos_ref, sin_ref, gain_ref, wq_hbm, wk_hbm, wv_hbm, wo_hbm, wg_hbm, wu_hbm, wd_hbm, k_hbm, v_hbm, y_ref,
                 xbuf, wq, wk, wv, wo, wg, wu, wd, kbuf, vbuf, sbuf, part, red1, red2, mbuf, mid, act, x_sem, w_sem, kv_sem, send_sem, recv_sem):
    t = lax.axis_index('t')
    v = lax.axis_index('v')
    tp, piece = 4, y_ref.shape[1]
    rows = tp * piece
    block = CHUNKS * piece
    width = x_hbm.shape[1]
    half = width // 2
    head = wk.shape[1]
    ctx = kbuf.shape[0] // rows
    score_scale = head ** -0.5

    def token0(c, o):
        return tp * block * v + block * o + piece * c

    x_copies = []
    for c in range(CHUNKS):
        for o in range(tp):
            x_copies.append(pltpu.make_async_copy(x_hbm.at[pl.ds(pl.multiple_of(token0(c, o), piece), piece)], xbuf.at[c, pl.ds(o * piece, piece)], x_sem.at[c, o]))

    def kv_copies(c):
        out = []
        for o in range(tp):
            src = pl.ds(pl.multiple_of(token0(c, o) * ctx, piece * ctx), piece * ctx)
            dst = pl.ds(o * piece * ctx, piece * ctx)
            out.append(pltpu.make_async_copy(k_hbm.at[src], kbuf.at[dst], kv_sem.at[c, 0, o]))
            out.append(pltpu.make_async_copy(v_hbm.at[src], vbuf.at[dst], kv_sem.at[c, 1, o]))
        return out

    pairs = ((wq_hbm, wq), (wk_hbm, wk), (wv_hbm, wv), (wo_hbm, wo), (wg_hbm, wg), (wu_hbm, wu), (wd_hbm, wd))
    w_copies = [pltpu.make_async_copy(src, dst, w_sem.at[i]) for i, (src, dst) in enumerate(pairs)]
    for cp in x_copies[:tp]:
        cp.start()
    for cp in w_copies[:3]:
        cp.start()
    for cp in kv_copies(0):
        cp.start()
    w_copies[3].start()
    for cp in x_copies[tp:]:
        cp.start()
    for cp in w_copies[4:]:
        cp.start()

    barrier = pltpu.get_barrier_semaphore()
    for mask in (1, 2):
        pl.semaphore_signal(barrier, inc=1, device_id=(flip_t(t, mask), v), device_id_type=MESH)

    def attend(c):
        for cp in x_copies[c * tp:(c + 1) * tp]:
            cp.wait()
        a = rms(xbuf[c].astype(F32), gain_ref[0:1, :]).astype(BF16)
        if c == 0:
            for cp in w_copies[:3]:
                cp.wait()
        q = jnp.dot(a, wq[...], preferred_element_type=F32)
        k = jnp.dot(a, wk[...], preferred_element_type=F32)
        val = jnp.dot(a, wv[...], preferred_element_type=F32).astype(BF16).astype(F32)
        cos_t = cos_ref[c * rows:(c + 1) * rows, :]
        sin_t = sin_ref[c * rows:(c + 1) * rows, :]

        def rope(z):
            low, high = z[:, :head // 2], z[:, head // 2:]
            return jnp.concatenate([low * cos_t - high * sin_t, high * cos_t + low * sin_t], axis=1).astype(BF16).astype(F32)

        q0, q1, k = rope(q[:, :head]), rope(q[:, head:]), rope(k)
        groups = rows // 8

        def by_group(first, second):
            return jnp.concatenate([piece8 for g in range(groups) for piece8 in (first[8 * g:8 * g + 8], second[8 * g:8 * g + 8])], axis=0)

        q_all = by_group(q0, q1)
        s_new = jnp.sum(q_all * by_group(k, k), axis=1, keepdims=True)
        val_all = by_group(val, val)
        q_bf = q_all.astype(BF16)
        for cp in kv_copies(c):
            cp.wait()
        for g in range(groups):
            sbuf[16 * g:16 * g + 16, :] = lax.dot_general(q_bf[16 * g:16 * g + 16], kbuf[8 * ctx * g:8 * ctx * (g + 1), :], (((1,), (1,)), ((), ())), preferred_element_type=F32)
        seq8 = seq_ref[c * rows:(c + 1) * rows, :]
        seq_all = by_group(seq8, seq8)
        seq_all = jnp.concatenate([seq_all] * (8 * ctx // 128), axis=1)
        lane = lax.broadcasted_iota(jnp.int32, (2 * rows, 8 * ctx), 1)
        row = lax.broadcasted_iota(jnp.int32, (2 * rows, 8 * ctx), 0)
        valid = jnp.logical_and(lane // ctx == row % 8, lane % ctx < seq_all)
        s = ATTN_CAP * jnp.tanh(sbuf[...] * (score_scale / ATTN_CAP))
        s_new = ATTN_CAP * jnp.tanh(s_new * (score_scale / ATTN_CAP))
        s = jnp.where(valid, s, -1e30)
        top = jnp.maximum(jnp.max(s, axis=1, keepdims=True), s_new)
        p = jnp.where(valid, jnp.exp(s - top), 0.0)
        p_new = jnp.exp(s_new - top)
        denom = jnp.sum(p, axis=1, keepdims=True) + p_new
        p_bf = p.astype(BF16)
        for g in range(groups):
            sbuf[16 * g:16 * g + 16, :head] = jnp.dot(p_bf[16 * g:16 * g + 16], vbuf[8 * ctx * g:8 * ctx * (g + 1), :], preferred_element_type=F32)
        o_all = (sbuf[:, :head] + p_new.astype(BF16).astype(F32) * val_all) / denom
        o0 = jnp.concatenate([o_all[16 * g:16 * g + 8] for g in range(groups)], axis=0)
        o1 = jnp.concatenate([o_all[16 * g + 8:16 * g + 16] for g in range(groups)], axis=0)
        if c + 1 < CHUNKS:
            for cp in kv_copies(c + 1):
                cp.start()
        if c == 0:
            w_copies[3].wait()
        o = jnp.concatenate([o0, o1], axis=1).astype(BF16)
        part[c] = jnp.dot(o, wo[...], preferred_element_type=F32)

    order = ((2, 1), (1, 2))

    def cols(h):
        return pl.ds(h * half, half)

    def rows_of(o):
        return pl.ds(pl.multiple_of(o * piece, piece), piece)

    def remote(src, dst, c, phase, h, i, mask):
        return pltpu.make_async_remote_copy(src_ref=src, dst_ref=dst, send_sem=send_sem.at[c, phase, h, i], recv_sem=recv_sem.at[c, phase, h, i],
                                            device_id=(flip_t(t, mask), v), device_id_type=MESH)

    def scatter1(c, phase, h, i):
        m1, m2 = order[h]
        owner = flip_t(t, 3) if i else flip_t(t, m1)
        return remote(part.at[c, rows_of(owner), cols(h)], red1.at[phase // 2, c, h, i], c, phase, h, i, m1)

    def scatter2(c, phase, h):
        return remote(red1.at[phase // 2, c, h, 1], red2.at[phase // 2, c, h], c, phase, h, 2, order[h][1])

    def scatter_start(c, phase):
        for i in (1, 0):
            for h in range(2):
                scatter1(c, phase, h, i).start()

    def scatter_pass(c, phase):
        for h in range(2):
            scatter1(c, phase, h, 1).wait_recv()
            red1[phase // 2, c, h, 1] = red1[phase // 2, c, h, 1] + part[c, rows_of(flip_t(t, order[h][1])), h * half:(h + 1) * half]
            scatter2(c, phase, h).start()

    def scatter_end(c, phase):
        got = []
        for h in range(2):
            scatter1(c, phase, h, 0).wait_recv()
            scatter2(c, phase, h).wait_recv()
            got.append(part[c, rows_of(t), h * half:(h + 1) * half] + red1[phase // 2, c, h, 0] + red2[phase // 2, c, h])
        for h in range(2):
            scatter1(c, phase, h, 0).wait_send()
            scatter1(c, phase, h, 1).wait_send()
            scatter2(c, phase, h).wait_send()
        return jnp.concatenate(got, axis=1)

    def gather(c, h, i):
        m1, m2 = order[h]
        where = mbuf.at[c, rows_of(flip_t(t, m2) if i == 2 else t), cols(h)]
        return remote(where, where, c, 1, h, i, m1 if i else m2)

    def gather_start(c):
        for i in (0, 1):
            for h in range(2):
                gather(c, h, i).start()

    def gather_pass(c):
        for h in range(2):
            gather(c, h, 0).wait_recv()
            gather(c, h, 2).start()

    def gather_end(c):
        for h in range(2):
            gather(c, h, 1).wait_recv()
            gather(c, h, 2).wait_recv()

    def gather_sent(c):
        for h in range(2):
            for i in range(3):
                gather(c, h, i).wait_send()

    def middle(c):
        attn_out = scatter_end(c, 0)
        x_own = xbuf[c, rows_of(t), :].astype(F32)
        x1 = (x_own + rms(attn_out, gain_ref[1:2, :])).astype(BF16).astype(F32)
        mid[c] = x1
        mbuf[c, rows_of(t), :] = rms(x1, gain_ref[2:3, :]).astype(BF16).astype(F32)

    def mlp(c):
        if c == 0:
            for cp in w_copies[4:]:
                cp.wait()
        m = mbuf[c].astype(BF16)
        tiles = 3
        wide = width // tiles

        def up_tile(i, carry):
            at = pl.ds(pl.multiple_of(i * wide, 128), wide)
            gate = jnp.dot(m, wg[:, at], preferred_element_type=F32)
            up = jnp.dot(m, wu[:, at], preferred_element_type=F32)
            act[:, at] = (jax.nn.gelu(gate, approximate=True) * up).astype(BF16)
            return carry

        lax.fori_loop(0, tiles, up_tile, 0)

        def down_tile(i, carry):
            at = pl.ds(pl.multiple_of(i * wide, 128), wide)
            part[c, :, at] = jnp.dot(act[...], wd[:, at], preferred_element_type=F32)
            return carry

        lax.fori_loop(0, tiles, down_tile, 0)

    attend(0)
    pl.semaphore_wait(barrier, 2)
    scatter_start(0, 0)
    attend(1)
    scatter_start(1, 0)
    scatter_pass(0, 0)
    scatter_pass(1, 0)
    middle(0)
    gather_start(0)
    middle(1)
    gather_start(1)
    gather_pass(0)
    gather_end(0)
    gather_pass(1)
    mlp(0)
    scatter_start(0, 2)
    gather_end(1)
    mlp(1)
    scatter_start(1, 2)
    scatter_pass(0, 2)
    scatter_pass(1, 2)
    for c in range(CHUNKS):
        y_ref[c] = (mid[c] + rms(scatter_end(c, 2), gain_ref[3:4, :])).astype(BF16).astype(F32)
        gather_sent(c)


def layer(tokens, x, seq_rows, cos_t, sin_t, gains, w_q, w_k, w_v, w_o, w_gate, w_up, w_down, k_rows, v_rows):
    width = x.shape[1]
    piece = tokens // 16 // CHUNKS
    rows = 4 * piece
    head = w_k.shape[1]
    ctx = k_rows.shape[0] // tokens
    ff = w_gate.shape[1]
    vm = pl.BlockSpec(memory_space=pltpu.VMEM)
    hbm = pl.BlockSpec(memory_space=pl.ANY)
    return pl.pallas_call(
        layer_kernel,
        out_shape=jax.ShapeDtypeStruct((CHUNKS, piece, width), F32),
        in_specs=[hbm] + [vm] * 4 + [hbm] * 9,
        out_specs=vm,
        scratch_shapes=[
            pltpu.VMEM((CHUNKS, rows, width), BF16),
            *[pltpu.VMEM(w.shape, BF16) for w in (w_q, w_k, w_v, w_o, w_gate, w_up, w_down)],
            pltpu.VMEM((rows * ctx, head), BF16),
            pltpu.VMEM((rows * ctx, head), BF16),
            pltpu.VMEM((2 * rows, 8 * ctx), F32),
            pltpu.VMEM((CHUNKS, rows, width), F32),
            pltpu.VMEM((2, CHUNKS, 2, 2, piece, width // 2), F32),
            pltpu.VMEM((2, CHUNKS, 2, piece, width // 2), F32),
            pltpu.VMEM((CHUNKS, rows, width), F32),
            pltpu.VMEM((CHUNKS, piece, width), F32),
            pltpu.VMEM((rows, ff), BF16),
            pltpu.SemaphoreType.DMA((CHUNKS, 4)),
            pltpu.SemaphoreType.DMA((7,)),
            pltpu.SemaphoreType.DMA((CHUNKS, 2, 4)),
            pltpu.SemaphoreType.DMA((CHUNKS, 3, 2, 3)),
            pltpu.SemaphoreType.DMA((CHUNKS, 3, 2, 3)),
        ],
        compiler_params=pltpu.CompilerParams(collective_id=0, has_side_effects=True, vmem_limit_bytes=66_000_000),
        name='layer',
    )(x, seq_rows, cos_t, sin_t, gains, w_q, w_k, w_v, w_o, w_gate, w_up, w_down, k_rows, v_rows)


AXES = ('x', 'z', 'y')
FLIP = {'x': (0, 2), 'y': (1, 0), 'z': (2, 0), 'c': (0, 1)}


def head_kernel(y_own, gain_ref, tgt_ref, e_hbm, logp_ref, y_hbm,
                ybuf, hbuf, ystage, ebuf, lg0, lg1, stat, stats, e_sem, y_sem, send_sem, recv_sem, stat_send, stat_recv):
    t = lax.axis_index('t')
    v = lax.axis_index('v')
    me = 4 * v + t
    piece, width = y_own.shape[1:]
    toks = 16 * piece
    third = width // 3
    sub = E_ROWS // 2
    vocab_local = e_hbm.shape[0]
    tiles = vocab_local // E_ROWS
    total = tiles * CHUNKS

    barrier = pltpu.get_barrier_semaphore()
    for j in range(1, 16):
        other = (me + j) % 16
        pl.semaphore_signal(barrier, inc=1, device_id=(other % 4, other // 4), device_id_type=MESH)

    def e_copy(i):
        tile = i % tiles
        slot = i % E_SLOTS
        return pltpu.make_async_copy(e_hbm.at[pl.ds(pl.multiple_of(tile * E_ROWS, E_ROWS), E_ROWS)], ebuf.at[slot], e_sem.at[slot])

    for i in range(E_SLOTS - 1):
        e_copy(i).start()
    for c in range(CHUNKS):
        ybuf[c, pl.ds(pl.multiple_of(me * piece, piece), piece), :] = y_own[c]
    lg1[...] = jnp.zeros_like(lg1)
    pl.semaphore_wait(barrier, 15)

    def axes_of(p, bits):
        order = [AXES[(p + s) % 3] for s in range(3)]
        mt = mv = 0
        for s in range(3):
            if bits >> s & 1:
                mt ^= FLIP[order[s]][0]
                mv ^= FLIP[order[s]][1]
        return mt, mv

    def block_copy(c, p, s, bits):
        mt, mv = axes_of(p, bits)
        blk = 4 * flip_v(v, mv) + flip_t(t, mt)
        at = ybuf.at[c, pl.ds(pl.multiple_of(blk * piece, piece), piece), pl.ds(p * third, third)]
        src = y_own.at[c, :, pl.ds(p * third, third)] if bits == 0 else at
        ft, fv = FLIP['c'] if s == 3 else FLIP[AXES[(p + s) % 3]]
        i = 2 ** s - 1 + bits
        return pltpu.make_async_remote_copy(src_ref=src, dst_ref=at, send_sem=send_sem.at[c, p, i], recv_sem=recv_sem.at[c, p, i],
                                            device_id=(flip_t(t, ft), flip_v(v, fv)), device_id_type=MESH)

    def spread(c, step):
        if step == 0:
            for s in (0, 1, 2, 3):
                for p in range(3):
                    block_copy(c, p, s, 0).start()
        elif step <= 3:
            s = step - 1
            for bits in range(2 ** s):
                for p in range(3):
                    block_copy(c, p, s, bits).wait_recv()
                    for later in range(s + 1, 4):
                        block_copy(c, p, later, bits | 1 << s).start()
        else:
            for p in range(3):
                for bits in range(8):
                    block_copy(c, p, 3, bits).wait_recv()

    def spread_sent(c):
        for p in range(3):
            for s in range(4):
                for bits in range(2 ** s):
                    block_copy(c, p, s, bits).wait_send()

    def y_copy(c, b):
        return pltpu.make_async_copy(ystage.at[pl.ds(b * piece, piece)], y_hbm.at[pl.ds((b * CHUNKS + c) * piece, piece)], y_sem.at[c, b])

    def stat_copy(c, j):
        other = (me + j) % 16
        return pltpu.make_async_remote_copy(src_ref=stat.at[c], dst_ref=stats.at[c, me], send_sem=stat_send.at[c, j - 1], recv_sem=stat_recv.at[c, j - 1],
                                            device_id=(other % 4, other // 4), device_id_type=MESH)

    for step in range(5):
        spread(0, step)

    lanes = lax.broadcasted_iota(jnp.int32, (8, toks), 0)

    def reduce_rows(lg, first_row, tgt):
        rel = tgt - first_row
        s_acc = [jnp.zeros((8, toks), F32) for _ in range(2)]
        t_acc = [jnp.zeros((8, toks), F32) for _ in range(2)]
        for r in range(sub // 8):
            th = jnp.tanh(lg[8 * r:8 * r + 8, :] * (1.0 / FINAL_CAP))
            s_acc[r % 2] = s_acc[r % 2] + jnp.exp(th * FINAL_CAP)
            t_acc[r % 2] = t_acc[r % 2] + jnp.where(lanes == rel - 8 * r, th, 0.0)
        return s_acc[0] + s_acc[1], t_acc[0] + t_acc[1]

    for c in range(CHUNKS):
        strip = 128
        if c:
            for b in range(16):
                y_copy(c - 1, b).wait()
        for r in range(toks // strip):
            yv = ybuf[c, r * strip:(r + 1) * strip, :]
            ystage[r * strip:(r + 1) * strip, :] = yv.astype(BF16)
            hbuf[:, r * strip:(r + 1) * strip] = rms(yv, gain_ref[4:5, :]).T.astype(BF16)
        for b in range(16):
            y_copy(c, b).start()
        tgt = jnp.broadcast_to(tgt_ref[c], (8, toks)) - me * vocab_local
        if c + 1 < CHUNKS:
            spread(c + 1, 0)

        def step(i, carry):
            s_sum, t_sum = carry
            n = c * tiles + i

            @pl.when(n + E_SLOTS - 1 < total)
            def _():
                e_copy(n + E_SLOTS - 1).start()

            e_copy(n).wait()
            slot = n % E_SLOTS
            lg0[...] = jnp.dot(ebuf[slot, :sub, :], hbuf[...], preferred_element_type=F32)
            s_part, t_part = reduce_rows(lg1, i * E_ROWS - sub, tgt)
            keep = i > 0
            s_sum = s_sum + jnp.where(keep, s_part, 0.0)
            t_sum = t_sum + jnp.where(keep, t_part, 0.0)
            lg1[...] = jnp.dot(ebuf[slot, sub:, :], hbuf[...], preferred_element_type=F32)
            s_part, t_part = reduce_rows(lg0, i * E_ROWS, tgt)
            if c + 1 < CHUNKS:
                for stage, at in ((1, 3), (2, 6), (3, 10), (4, 13)):
                    @pl.when(i == at)
                    def _(stage=stage):
                        spread(c + 1, stage)
            return s_sum + s_part, t_sum + t_part

        zero = jnp.zeros((8, toks), F32)
        s_sum, t_sum = lax.fori_loop(0, tiles, step, (zero, zero))
        s_part, t_part = reduce_rows(lg1, tiles * E_ROWS - sub, tgt)
        s_sum = jnp.sum(s_sum + s_part, axis=0, keepdims=True)
        t_sum = jnp.sum(t_sum + t_part, axis=0, keepdims=True)
        both = jnp.where(lanes == 0, s_sum, jnp.where(lanes == 1, t_sum, 0.0))
        stat[c] = both
        stats[c, me] = both
        for j in range(1, 16):
            stat_copy(c, j).start()

    for c in range(CHUNKS):
        for j in range(1, 16):
            stat_copy(c, j).wait_recv()
        tot = stats[c, 0]
        for b in range(1, 16):
            tot = tot + stats[c, b]
        logp_ref[c] = FINAL_CAP * tot[1:2, :] - jnp.log(tot[0:1, :])
    for c in range(CHUNKS):
        spread_sent(c)
        for j in range(1, 16):
            stat_copy(c, j).wait_send()
    for b in range(16):
        y_copy(CHUNKS - 1, b).wait()


def head(tokens, y_own, gains, tgt, table):
    piece, width = y_own.shape[1:]
    toks = 16 * piece
    vm = pl.BlockSpec(memory_space=pltpu.VMEM)
    hbm = pl.BlockSpec(memory_space=pl.ANY)
    return pl.pallas_call(
        head_kernel,
        out_shape=(jax.ShapeDtypeStruct((CHUNKS, 1, toks), F32), jax.ShapeDtypeStruct((tokens, width), BF16)),
        in_specs=[vm, vm, vm, hbm],
        out_specs=(vm, hbm),
        scratch_shapes=[
            pltpu.VMEM((CHUNKS, toks, width), F32),
            pltpu.VMEM((width, toks), BF16),
            pltpu.VMEM((toks, width), BF16),
            pltpu.VMEM((E_SLOTS, E_ROWS, width), BF16),
            pltpu.VMEM((E_ROWS // 2, toks), F32),
            pltpu.VMEM((E_ROWS // 2, toks), F32),
            pltpu.VMEM((CHUNKS, 8, toks), F32),
            pltpu.VMEM((CHUNKS, 16, 8, toks), F32),
            pltpu.SemaphoreType.DMA((E_SLOTS,)),
            pltpu.SemaphoreType.DMA((CHUNKS, 16)),
            pltpu.SemaphoreType.DMA((CHUNKS, 3, 15)),
            pltpu.SemaphoreType.DMA((CHUNKS, 3, 15)),
            pltpu.SemaphoreType.DMA((CHUNKS, 15)),
            pltpu.SemaphoreType.DMA((CHUNKS, 15)),
        ],
        compiler_params=pltpu.CompilerParams(collective_id=1, has_side_effects=True, vmem_limit_bytes=60_000_000),
        name='head',
    )(y_own, gains, tgt, table)


def solution(mesh):
    in_specs = (P(), P(), P(), P(), P(None, 't'), P(None, 't'), P(None, 't'), P('t', None), P(), P(), P(None, 't'), P(None, 't'), P('t', None), P(), P(), P(None, None, 't', None), P(None, None, 't', None), P(('v', 't'), None))

    def local_step(hidden_in, seq_lens, target, g_attn_pre, w_q, w_k, w_v, w_o, g_attn_post, g_mlp_pre, w_gate, w_up, w_down, g_mlp_post, g_final, k_cache, v_cache, embed_table):
        tokens = hidden_in.shape[0]
        group = tokens // 4
        piece = tokens // 16 // CHUNKS
        ctx, _, head_dim = k_cache.shape[1:]
        half_dim = head_dim // 2
        gains = 1.0 + jnp.stack([g_attn_pre, g_attn_post, g_mlp_pre, g_mlp_post, g_final]).astype(F32)
        seq = lax.dynamic_slice(seq_lens, (lax.axis_index('v') * group,), (group,))
        seq = seq.reshape(4, CHUNKS, piece).transpose(1, 0, 2).reshape(group)
        inv_freq = ROPE_BASE ** (-2.0 * jnp.arange(half_dim, dtype=F32) / head_dim)
        angles = seq.astype(F32)[:, None] * inv_freq[None, :]
        seq_rows = jnp.broadcast_to(seq[:, None], (group, 128))
        k_rows = k_cache.reshape(tokens * ctx, head_dim)
        v_rows = v_cache.reshape(tokens * ctx, head_dim)
        y_own = layer(tokens, hidden_in, seq_rows, jnp.cos(angles), jnp.sin(angles), gains, w_q, w_k, w_v, w_o, w_gate, w_up, w_down, k_rows, v_rows)
        tgt = target.reshape(16, CHUNKS, piece).transpose(1, 0, 2).reshape(CHUNKS, 1, 16 * piece)
        logp, hidden_out = head(tokens, y_own, gains, tgt, embed_table)
        logprob = logp.reshape(CHUNKS, 16, piece).transpose(1, 0, 2).reshape(tokens)
        return logprob, hidden_out

    return jax.shard_map(local_step, mesh=mesh, in_specs=in_specs, out_specs=(P(), P()), check_vma=False)
```

```python
import jax
import jax.numpy as jnp
import numpy as np
from jax import lax
from jax.experimental import pallas as pl
from jax.experimental.pallas import tpu as pltpu
from jax.sharding import PartitionSpec as P

ATTN_CAP = 50.0
FINAL_CAP = 30.0
NORM_EPS = 1e-6
ROPE_BASE = 10000.0
MESH = pl.DeviceIdType.MESH
F32 = jnp.float32
BF16 = jnp.bfloat16

PIECES = (32, 32)
E_ROWS = 800
E_SLOTS = 8
AXES = ('x', 'z', 'y')
FLIP = {'x': (0, 2), 'y': (1, 0), 'z': (2, 0), 'c': (0, 1)}


def flip_t(t, mask):
    if mask == 0:
        return t
    if mask == 1:
        return t + 1 - 2 * (t % 2)
    if mask == 2:
        return (t + 2) % 4
    return 3 - t


def flip_v(v, mask):
    return flip_t(v, mask)


def rms(values, gain):
    return values * lax.rsqrt(jnp.mean(values * values, axis=-1, keepdims=True) + NORM_EPS) * gain


def kernel(x_hbm, seq_ref, tgt_ref, freq_ref, g_attn_pre, g_attn_post, g_mlp_pre, g_mlp_post, g_final,
           wq_hbm, wk_hbm, wv_hbm, wo_hbm, wg_hbm, wu_hbm, wd_hbm, k_hbm, v_hbm, e_hbm, logp_ref, y_hbm,
           xbuf, wq, wk, wv, wo, big, sbuf, part, red1, red2, ybuf, mid, act, lg0, lg1, stat, stats,
           x_sem, w_sem, kv_sem, e_sem, y_sem, send_sem, recv_sem, spread_send, spread_recv, stat_send, stat_recv):
    t = lax.axis_index('t')
    v = lax.axis_index('v')
    me = 4 * v + t
    chunks = len(PIECES)
    bases = [16 * sum(PIECES[:c]) for c in range(chunks)]
    width = x_hbm.shape[1]
    half, third = width // 2, width // 3
    ff = wg_hbm.shape[1]
    head = wk.shape[1]
    ctx = k_hbm.shape[0] // x_hbm.shape[0]
    score_scale = head ** -0.5
    groups_of = [4 * n for n in PIECES]
    toks_of = [16 * n for n in PIECES]

    def gain(ref):
        return 1.0 + ref[...].astype(F32).reshape(1, width)

    def group_rows(c):
        return pl.multiple_of(bases[c] + groups_of[c] * v, 8)

    x_copies = [pltpu.make_async_copy(x_hbm.at[pl.ds(group_rows(c), groups_of[c])], xbuf.at[c, pl.ds(0, groups_of[c])], x_sem.at[c]) for c in range(chunks)]

    def kv_at(c, i):
        return pl.ds(ff, groups_of[c] * ctx), pl.ds((2 * c + i) * head, head)

    def kv_copies(c):
        rows = pl.ds(pl.multiple_of(group_rows(c) * ctx, 8 * ctx), groups_of[c] * ctx)
        return [pltpu.make_async_copy(src.at[rows], big.at[kv_at(c, i)], kv_sem.at[c, i]) for i, src in enumerate((k_hbm, v_hbm))]

    pairs = ((wq_hbm, wq), (wk_hbm, wk), (wv_hbm, wv), (wo_hbm, wo), (wg_hbm, big.at[pl.ds(0, width)]), (wu_hbm, big.at[pl.ds(width, width)]), (wd_hbm, big.at[pl.ds(2 * width, ff)]))
    w_copies = [pltpu.make_async_copy(src, dst, w_sem.at[i]) for i, (src, dst) in enumerate(pairs)]
    x_copies[0].start()
    for cp in w_copies[:3]:
        cp.start()
    for cp in kv_copies(0):
        cp.start()
    w_copies[3].start()
    for c in range(1, chunks):
        x_copies[c].start()
        for cp in kv_copies(c):
            cp.start()
    w_copies[4].start()

    barrier = pltpu.get_barrier_semaphore()
    for j in range(1, 16):
        other = (me + j) % 16
        pl.semaphore_signal(barrier, inc=1, device_id=(other % 4, other // 4), device_id_type=MESH)

    def attend(c):
        rows = groups_of[c]
        x_copies[c].wait()
        a = rms(xbuf[c, :rows, :].astype(F32), gain(g_attn_pre)).astype(BF16)
        if c == 0:
            for cp in w_copies[:3]:
                cp.wait()
        q = jnp.dot(a, wq[...], preferred_element_type=F32)
        k = jnp.dot(a, wk[...], preferred_element_type=F32)
        val = jnp.dot(a, wv[...], preferred_element_type=F32).astype(BF16).astype(F32)
        start = group_rows(c)
        seq_row = seq_ref[pl.ds(start // 128, 1), :]
        lane = lax.broadcasted_iota(jnp.int32, (rows, 128), 1)
        row = lax.broadcasted_iota(jnp.int32, (rows, 128), 0)
        pos = jnp.sum(jnp.where(lane == row + start % 128, seq_row.astype(F32), 0.0), axis=1, keepdims=True)
        angle = pos * freq_ref[...]
        cos_t, sin_t = jnp.cos(angle), jnp.sin(angle)

        def rope(z):
            low, high = z[:, :head // 2], z[:, head // 2:]
            return jnp.concatenate([low * cos_t - high * sin_t, high * cos_t + low * sin_t], axis=1).astype(BF16).astype(F32)

        q0, q1, k = rope(q[:, :head]), rope(q[:, head:]), rope(k)
        groups = rows // 8

        def by_group(first, second):
            return jnp.concatenate([part8 for g in range(groups) for part8 in (first[8 * g:8 * g + 8], second[8 * g:8 * g + 8])], axis=0)

        q_all = by_group(q0, q1)
        s_new = jnp.sum(q_all * by_group(k, k), axis=1, keepdims=True)
        val_all = by_group(val, val)
        q_bf = q_all.astype(BF16)
        pos_all = by_group(pos, pos).astype(jnp.int32)
        for cp in kv_copies(c):
            cp.wait()

        def cached(i, g):
            return big[ff + 8 * ctx * g:ff + 8 * ctx * (g + 1), (2 * c + i) * head:(2 * c + i + 1) * head]

        for g in range(groups):
            sbuf[16 * g:16 * g + 16, :] = lax.dot_general(q_bf[16 * g:16 * g + 16], cached(0, g), (((1,), (1,)), ((), ())), preferred_element_type=F32)
        lane = lax.broadcasted_iota(jnp.int32, (2 * rows, 8 * ctx), 1)
        row = lax.broadcasted_iota(jnp.int32, (2 * rows, 8 * ctx), 0)
        valid = jnp.logical_and(lane // ctx == row % 8, lane % ctx < pos_all)
        s = ATTN_CAP * jnp.tanh(sbuf[:2 * rows, :] * (score_scale / ATTN_CAP))
        s_new = ATTN_CAP * jnp.tanh(s_new * (score_scale / ATTN_CAP))
        s = jnp.where(valid, s, -1e30)
        top = jnp.maximum(jnp.max(s, axis=1, keepdims=True), s_new)
        p = jnp.where(valid, jnp.exp(s - top), 0.0)
        p_new = jnp.exp(s_new - top)
        denom = jnp.sum(p, axis=1, keepdims=True) + p_new
        p_bf = p.astype(BF16)
        for g in range(groups):
            sbuf[16 * g:16 * g + 16, :head] = jnp.dot(p_bf[16 * g:16 * g + 16], cached(1, g), preferred_element_type=F32)
        o_all = (sbuf[:2 * rows, :head] + p_new.astype(BF16).astype(F32) * val_all) / denom
        o0 = jnp.concatenate([o_all[16 * g:16 * g + 8] for g in range(groups)], axis=0)
        o1 = jnp.concatenate([o_all[16 * g + 8:16 * g + 16] for g in range(groups)], axis=0)
        if c == 0:
            w_copies[3].wait()
        o = jnp.concatenate([o0, o1], axis=1).astype(BF16)
        part[c, :rows, :] = jnp.dot(o, wo[...], preferred_element_type=F32)
        if c + 1 == chunks:
            for cp in w_copies[5:]:
                cp.start()

    order = ((2, 1), (1, 2))

    def cols(h):
        return pl.ds(h * half, half)

    def rows_of(c, o):
        return pl.ds(pl.multiple_of(o * PIECES[c], 8), PIECES[c])

    def y_rows(c, o):
        return pl.ds(pl.multiple_of(group_rows(c) + o * PIECES[c], 8), PIECES[c])

    def remote(src, dst, c, phase, h, i, mask):
        return pltpu.make_async_remote_copy(src_ref=src, dst_ref=dst, send_sem=send_sem.at[c, phase, h, i], recv_sem=recv_sem.at[c, phase, h, i],
                                            device_id=(flip_t(t, mask), v), device_id_type=MESH)

    def scatter1(c, phase, h, i):
        m1, m2 = order[h]
        owner = flip_t(t, 3) if i else flip_t(t, m1)
        return remote(part.at[c, rows_of(c, owner), cols(h)], red1.at[c, h, i, pl.ds(0, PIECES[c])], c, phase, h, i, m1)

    def scatter2(c, phase, h):
        return remote(red1.at[c, h, 1, pl.ds(0, PIECES[c])], red2.at[c, h, pl.ds(0, PIECES[c])], c, phase, h, 2, order[h][1])

    def scatter_start(c, phase):
        for i in (1, 0):
            for h in range(2):
                scatter1(c, phase, h, i).start()

    def scatter_pass(c, phase):
        n = PIECES[c]
        for h in range(2):
            scatter1(c, phase, h, 1).wait_recv()
            red1[c, h, 1, :n] = red1[c, h, 1, :n] + part[c, rows_of(c, flip_t(t, order[h][1])), h * half:(h + 1) * half]
            scatter2(c, phase, h).start()

    def scatter_end(c, phase):
        n = PIECES[c]
        got = []
        for h in range(2):
            scatter1(c, phase, h, 0).wait_recv()
            scatter2(c, phase, h).wait_recv()
            got.append(part[c, rows_of(c, t), h * half:(h + 1) * half] + red1[c, h, 0, :n] + red2[c, h, :n])
        for h in range(2):
            scatter1(c, phase, h, 0).wait_send()
            scatter1(c, phase, h, 1).wait_send()
            scatter2(c, phase, h).wait_send()
        return jnp.concatenate(got, axis=1)

    def gather(c, h, i):
        m1, m2 = order[h]
        where = ybuf.at[y_rows(c, flip_t(t, m2) if i == 2 else t), cols(h)]
        return remote(where, where, c, 1, h, i, m1 if i else m2)

    def gather_start(c):
        for i in (0, 1):
            for h in range(2):
                gather(c, h, i).start()

    def gather_pass(c):
        for h in range(2):
            gather(c, h, 0).wait_recv()
            gather(c, h, 2).start()

    def gather_end(c):
        for h in range(2):
            gather(c, h, 1).wait_recv()
            gather(c, h, 2).wait_recv()
        for h in range(2):
            for i in range(3):
                gather(c, h, i).wait_send()

    def middle(c):
        attn_out = scatter_end(c, 0)
        x_own = xbuf[c, rows_of(c, t), :].astype(F32)
        x1 = (x_own + rms(attn_out, gain(g_attn_post))).astype(BF16).astype(F32)
        mid[c, :PIECES[c]] = x1
        ybuf[y_rows(c, t), :] = rms(x1, gain(g_mlp_pre)).astype(BF16).astype(F32)
        gather_start(c)

    def mlp(c):
        rows = groups_of[c]
        gather_end(c)
        if c == 0:
            for cp in w_copies[4:]:
                cp.wait()
        m = ybuf[pl.ds(group_rows(c), rows), :].astype(BF16)
        tiles = 3
        wide = ff // tiles

        def up_tile(i, carry):
            at = pl.ds(pl.multiple_of(i * wide, 128), wide)
            gate = jnp.dot(m, big[:width, at], preferred_element_type=F32)
            up = jnp.dot(m, big[width:2 * width, at], preferred_element_type=F32)
            act[:rows, at] = (jax.nn.gelu(gate, approximate=True) * up).astype(BF16)
            return carry

        lax.fori_loop(0, tiles, up_tile, 0)

        def down_tile(i, carry):
            at = pl.ds(pl.multiple_of(i * wide, 128), wide)
            part[c, :rows, at] = jnp.dot(act[:rows, :], big[2 * width:2 * width + ff, at], preferred_element_type=F32)
            return carry

        lax.fori_loop(0, tiles, down_tile, 0)
        scatter_start(c, 2)

    def finish(c):
        y = (mid[c, :PIECES[c]] + rms(scatter_end(c, 2), gain(g_mlp_post))).astype(BF16).astype(F32)
        ybuf[y_rows(c, t), :] = y
        spread(c, 0)

    def axes_of(p, bits):
        axes = [AXES[(p + s) % 3] for s in range(3)]
        mt = mv = 0
        for s in range(3):
            if bits >> s & 1:
                mt ^= FLIP[axes[s]][0]
                mv ^= FLIP[axes[s]][1]
        return mt, mv

    def block_copy(c, p, s, bits):
        mt, mv = axes_of(p, bits)
        blk = 4 * flip_v(v, mv) + flip_t(t, mt)
        at = ybuf.at[pl.ds(pl.multiple_of(bases[c] + blk * PIECES[c], 8), PIECES[c]), pl.ds(p * third, third)]
        ft, fv = FLIP['c'] if s == 3 else FLIP[AXES[(p + s) % 3]]
        i = 2 ** s - 1 + bits
        return pltpu.make_async_remote_copy(src_ref=at, dst_ref=at, send_sem=spread_send.at[c, p, i], recv_sem=spread_recv.at[c, p, i],
                                            device_id=(flip_t(t, ft), flip_v(v, fv)), device_id_type=MESH)

    def spread(c, step):
        if step == 0:
            for s in (0, 1, 2, 3):
                for p in range(3):
                    block_copy(c, p, s, 0).start()
        elif step <= 3:
            s = step - 1
            for bits in range(2 ** s):
                for p in range(3):
                    block_copy(c, p, s, bits).wait_recv()
                    for later in range(s + 1, 4):
                        block_copy(c, p, later, bits | 1 << s).start()
        else:
            for p in range(3):
                for bits in range(8):
                    block_copy(c, p, 3, bits).wait_recv()

    def spread_sent(c):
        for p in range(3):
            for s in range(4):
                for bits in range(2 ** s):
                    block_copy(c, p, s, bits).wait_send()

    sub = E_ROWS // 2
    vocab_local = e_hbm.shape[0]
    tiles = vocab_local // E_ROWS
    total = tiles * chunks

    def e_copy(i):
        return pltpu.make_async_copy(e_hbm.at[pl.ds(pl.multiple_of(i % tiles * E_ROWS, E_ROWS), E_ROWS)],
                                     big.at[pl.ds(pl.multiple_of(i % E_SLOTS * E_ROWS, E_ROWS), E_ROWS)], e_sem.at[i % E_SLOTS])

    def y_copy(c):
        return pltpu.make_async_copy(wo.at[pl.ds(0, toks_of[c])], y_hbm.at[pl.ds(bases[c], toks_of[c])], y_sem.at[c])

    def stat_copy(c, j):
        other = (me + j) % 16
        return pltpu.make_async_remote_copy(src_ref=stat.at[c], dst_ref=stats.at[c, me], send_sem=stat_send.at[c, j - 1], recv_sem=stat_recv.at[c, j - 1],
                                            device_id=(other % 4, other // 4), device_id_type=MESH)

    def reduce_rows(lg, toks, tgt, first_row):
        rel = tgt - first_row
        sublane = lax.broadcasted_iota(jnp.int32, (8, toks), 0)
        s_acc = [jnp.zeros((8, toks), F32) for _ in range(2)]
        t_acc = [jnp.zeros((8, toks), F32) for _ in range(2)]
        for r in range(sub // 8):
            th = jnp.tanh(lg[8 * r:8 * r + 8, :toks] * (1.0 / FINAL_CAP))
            s_acc[r % 2] = s_acc[r % 2] + jnp.exp(th * FINAL_CAP)
            t_acc[r % 2] = t_acc[r % 2] + jnp.where(sublane == rel - 8 * r, th, 0.0)
        return s_acc[0] + s_acc[1], t_acc[0] + t_acc[1]

    def head_pass(c, tasks):
        toks = toks_of[c]
        strip = 128
        if c:
            y_copy(c - 1).wait()
        for r in range(toks // strip):
            yv = ybuf[bases[c] + r * strip:bases[c] + (r + 1) * strip, :]
            wo[r * strip:(r + 1) * strip, :] = yv.astype(BF16)
            wq[:, r * strip:(r + 1) * strip] = rms(yv, gain(g_final)).T.astype(BF16)
        y_copy(c).start()
        first = bases[c] // 128
        tgt = jnp.concatenate([tgt_ref[first + q:first + q + 1, :] for q in range(toks // 128)], axis=1)
        tgt = jnp.broadcast_to(tgt, (8, toks)) - me * vocab_local

        def step(i, carry):
            s_sum, t_sum = carry
            n = c * tiles + i
            slot = n % E_SLOTS * E_ROWS
            e_copy(n).wait()
            lg0[:, :toks] = jnp.dot(big[pl.ds(pl.multiple_of(slot, E_ROWS // 2), sub), :], wq[:, :toks], preferred_element_type=F32)
            s_part, t_part = reduce_rows(lg1, toks, tgt, i * E_ROWS - sub)
            keep = i > 0
            s_sum = s_sum + jnp.where(keep, s_part, 0.0)
            t_sum = t_sum + jnp.where(keep, t_part, 0.0)
            lg1[:, :toks] = jnp.dot(big[pl.ds(pl.multiple_of(slot + sub, E_ROWS // 2), sub), :], wq[:, :toks], preferred_element_type=F32)
            s_part, t_part = reduce_rows(lg0, toks, tgt, i * E_ROWS)

            @pl.when(n + E_SLOTS < total)
            def _():
                e_copy(n + E_SLOTS).start()

            for at, task in tasks:
                @pl.when(i == at)
                def _(task=task):
                    task()

            return s_sum + s_part, t_sum + t_part

        zero = jnp.zeros((8, toks), F32)
        s_sum, t_sum = lax.fori_loop(0, tiles, step, (zero, zero))
        s_part, t_part = reduce_rows(lg1, toks, tgt, tiles * E_ROWS - sub)
        s_sum = jnp.sum(s_sum + s_part, axis=0, keepdims=True)
        t_sum = jnp.sum(t_sum + t_part, axis=0, keepdims=True)
        sublane = lax.broadcasted_iota(jnp.int32, (8, toks), 0)
        both = jnp.where(sublane == 0, s_sum, jnp.where(sublane == 1, t_sum, 0.0))
        stat[c, :, :toks] = both
        stats[c, me, :, :toks] = both
        for j in range(1, 16):
            stat_copy(c, j).start()

    def combine(c):
        for j in range(1, 16):
            stat_copy(c, j).wait_recv()
        tot = stats[c, 0]
        for b in range(1, 16):
            tot = tot + stats[c, b]
        lp = FINAL_CAP * tot[1:2, :] - jnp.log(tot[0:1, :])
        for q in range(toks_of[c] // 128):
            logp_ref[bases[c] // 128 + q:bases[c] // 128 + q + 1, :] = lp[:, 128 * q:128 * (q + 1)]

    attend(0)
    lg1[...] = jnp.zeros_like(lg1)
    pl.semaphore_wait(barrier, 15)
    scatter_start(0, 0)
    attend(1)
    scatter_pass(0, 0)
    scatter_start(1, 0)
    middle(0)
    scatter_pass(1, 0)
    gather_pass(0)
    middle(1)
    mlp(0)
    gather_pass(1)
    scatter_pass(0, 2)
    mlp(1)
    for i in range(E_SLOTS):
        e_copy(i).start()
    finish(0)
    scatter_pass(1, 2)
    spread(0, 1)
    spread(0, 2)
    spread(0, 3)
    spread(0, 4)
    head_pass(0, ((0, lambda: finish(1)), (3, lambda: spread(1, 1)), (6, lambda: spread(1, 2)), (10, lambda: spread(1, 3)), (13, lambda: spread(1, 4))))
    head_pass(1, ((2, lambda: combine(0)),))
    combine(1)
    for c in range(chunks):
        spread_sent(c)
        for j in range(1, 16):
            stat_copy(c, j).wait_send()
    y_copy(chunks - 1).wait()


def step_kernel(x, seq, tgt, freq, gains, w_q, w_k, w_v, w_o, w_gate, w_up, w_down, k_rows, v_rows, table):
    tokens, width = x.shape
    chunks = len(PIECES)
    top = max(PIECES)
    rows, toks = 4 * top, 16 * top
    head = w_k.shape[1]
    ctx = k_rows.shape[0] // tokens
    ff = w_gate.shape[1]
    vm = pl.BlockSpec(memory_space=pltpu.VMEM)
    hbm = pl.BlockSpec(memory_space=pl.ANY)
    dma = pltpu.SemaphoreType.DMA
    return pl.pallas_call(
        kernel,
        out_shape=(jax.ShapeDtypeStruct((tokens // 128, 128), F32), jax.ShapeDtypeStruct((tokens, width), BF16)),
        in_specs=[hbm] + [vm] * 8 + [hbm] * 10,
        out_specs=(vm, hbm),
        scratch_shapes=[
            pltpu.VMEM((chunks, rows, width), BF16),
            pltpu.VMEM(w_q.shape, BF16),
            pltpu.VMEM(w_k.shape, BF16),
            pltpu.VMEM(w_v.shape, BF16),
            pltpu.VMEM(w_o.shape, BF16),
            pltpu.VMEM((2 * width + ff, ff), BF16),
            pltpu.VMEM((2 * rows, 8 * ctx), F32),
            pltpu.VMEM((chunks, rows, width), F32),
            pltpu.VMEM((chunks, 2, 2, top, width // 2), F32),
            pltpu.VMEM((chunks, 2, top, width // 2), F32),
            pltpu.VMEM((tokens, width), F32),
            pltpu.VMEM((chunks, top, width), F32),
            pltpu.VMEM((rows, ff), BF16),
            pltpu.VMEM((E_ROWS // 2, toks), F32),
            pltpu.VMEM((E_ROWS // 2, toks), F32),
            pltpu.VMEM((chunks, 8, toks), F32),
            pltpu.VMEM((chunks, 16, 8, toks), F32),
            dma((chunks,)),
            dma((7,)),
            dma((chunks, 2)),
            dma((E_SLOTS,)),
            dma((chunks,)),
            dma((chunks, 3, 2, 3)),
            dma((chunks, 3, 2, 3)),
            dma((chunks, 3, 15)),
            dma((chunks, 3, 15)),
            dma((chunks, 15)),
            dma((chunks, 15)),
        ],
        compiler_params=pltpu.CompilerParams(collective_id=0, has_side_effects=True, vmem_limit_bytes=67_000_000),
        name='step',
    )(x, seq, tgt, freq, *gains, w_q, w_k, w_v, w_o, w_gate, w_up, w_down, k_rows, v_rows, table)


def solution(mesh):
    in_specs = (P(), P(), P(), P(), P(None, 't'), P(None, 't'), P(None, 't'), P('t', None), P(), P(), P(None, 't'), P(None, 't'), P('t', None), P(), P(), P(None, None, 't', None), P(None, None, 't', None), P(('v', 't'), None))

    def local_step(hidden_in, seq_lens, target, g_attn_pre, w_q, w_k, w_v, w_o, g_attn_post, g_mlp_pre, w_gate, w_up, w_down, g_mlp_post, g_final, k_cache, v_cache, embed_table):
        tokens = hidden_in.shape[0]
        ctx, _, head_dim = k_cache.shape[1:]
        freq = ROPE_BASE ** (-2.0 * np.arange(head_dim // 2, dtype=np.float32) / head_dim)
        logp, hidden_out = step_kernel(
            hidden_in, seq_lens.reshape(-1, 128), target.reshape(-1, 128), jnp.asarray(freq[None, :], F32),
            (g_attn_pre, g_attn_post, g_mlp_pre, g_mlp_post, g_final), w_q, w_k, w_v, w_o, w_gate, w_up, w_down,
            k_cache.reshape(tokens * ctx, head_dim), v_cache.reshape(tokens * ctx, head_dim), embed_table)
        return logp.reshape(tokens), hidden_out

    return jax.shard_map(local_step, mesh=mesh, in_specs=in_specs, out_specs=(P(), P()), check_vma=False)
```

```python
import jax
import jax.numpy as jnp
import numpy as np
from jax import lax
from jax.experimental import pallas as pl
from jax.experimental.pallas import tpu as pltpu
from jax.sharding import PartitionSpec as P

ATTN_CAP = 50.0
FINAL_CAP = 30.0
NORM_EPS = 1e-6
ROPE_BASE = 10000.0
MESH = pl.DeviceIdType.MESH
F32 = jnp.float32
BF16 = jnp.bfloat16

PIECES = (32, 32)
E_ROWS = 1600
E_SLOTS = 4
AXES = ('x', 'z', 'y')
FLIP = {'x': (0, 2), 'y': (1, 0), 'z': (2, 0), 'c': (0, 1)}


def flip_t(t, mask):
    if mask == 0:
        return t
    if mask == 1:
        return t + 1 - 2 * (t % 2)
    if mask == 2:
        return (t + 2) % 4
    return 3 - t


def flip_v(v, mask):
    return flip_t(v, mask)


def rms(values, gain):
    return values * lax.rsqrt(jnp.mean(values * values, axis=-1, keepdims=True) + NORM_EPS) * gain


def kernel(x_hbm, seq_ref, tgt_ref, freq_ref, g_attn_pre, g_attn_post, g_mlp_pre, g_mlp_post, g_final,
           wq_hbm, wk_hbm, wv_hbm, wo_hbm, wg_hbm, wu_hbm, wd_hbm, k_hbm, v_hbm, e_hbm, logp_ref, y_hbm,
           xbuf, wq, wk, wv, wo, big, sbuf, part, red1, red2, ybuf, mid, act, lg0, lg1, stat, stats,
           x_sem, w_sem, kv_sem, e_sem, y_sem, send_sem, recv_sem, spread_send, spread_recv, stat_send, stat_recv):
    t = lax.axis_index('t')
    v = lax.axis_index('v')
    me = 4 * v + t
    chunks = len(PIECES)
    bases = [16 * sum(PIECES[:c]) for c in range(chunks)]
    width = x_hbm.shape[1]
    half, third = width // 2, width // 3
    ff = wg_hbm.shape[1]
    head = wk.shape[1]
    ctx = k_hbm.shape[0] // x_hbm.shape[0]
    score_scale = head ** -0.5
    groups_of = [4 * n for n in PIECES]
    toks_of = [16 * n for n in PIECES]

    def gain(ref):
        return 1.0 + ref[...].astype(F32).reshape(1, width)

    def group_rows(c):
        return pl.multiple_of(bases[c] + groups_of[c] * v, 8)

    x_copies = [pltpu.make_async_copy(x_hbm.at[pl.ds(group_rows(c), groups_of[c])], xbuf.at[c, pl.ds(0, groups_of[c])], x_sem.at[c]) for c in range(chunks)]

    def kv_at(c, i):
        return pl.ds(ff, groups_of[c] * ctx), pl.ds((2 * c + i) * head, head)

    def kv_copies(c):
        rows = pl.ds(pl.multiple_of(group_rows(c) * ctx, 8 * ctx), groups_of[c] * ctx)
        return [pltpu.make_async_copy(src.at[rows], big.at[kv_at(c, i)], kv_sem.at[c, i]) for i, src in enumerate((k_hbm, v_hbm))]

    pairs = ((wq_hbm, wq), (wk_hbm, wk), (wv_hbm, wv), (wo_hbm, wo), (wg_hbm, big.at[pl.ds(0, width)]), (wu_hbm, big.at[pl.ds(width, width)]), (wd_hbm, big.at[pl.ds(2 * width, ff)]))
    w_copies = [pltpu.make_async_copy(src, dst, w_sem.at[i]) for i, (src, dst) in enumerate(pairs)]
    x_copies[0].start()
    for cp in w_copies[:3]:
        cp.start()
    for cp in kv_copies(0):
        cp.start()
    w_copies[3].start()
    for c in range(1, chunks):
        x_copies[c].start()
        for cp in kv_copies(c):
            cp.start()
    w_copies[4].start()

    barrier = pltpu.get_barrier_semaphore()
    for j in range(1, 16):
        other = (me + j) % 16
        pl.semaphore_signal(barrier, inc=1, device_id=(other % 4, other // 4), device_id_type=MESH)

    def attend(c):
        rows = groups_of[c]
        x_copies[c].wait()
        a = rms(xbuf[c, :rows, :].astype(F32), gain(g_attn_pre)).astype(BF16)
        if c == 0:
            for cp in w_copies[:3]:
                cp.wait()
        q = jnp.dot(a, wq[...], preferred_element_type=F32)
        k = jnp.dot(a, wk[...], preferred_element_type=F32)
        val = jnp.dot(a, wv[...], preferred_element_type=F32).astype(BF16).astype(F32)
        start = group_rows(c)
        seq_row = seq_ref[pl.ds(start // 128, 1), :]
        lane = lax.broadcasted_iota(jnp.int32, (rows, 128), 1)
        row = lax.broadcasted_iota(jnp.int32, (rows, 128), 0)
        pos = jnp.sum(jnp.where(lane == row + start % 128, seq_row.astype(F32), 0.0), axis=1, keepdims=True)
        angle = pos * freq_ref[...]
        cos_t, sin_t = jnp.cos(angle), jnp.sin(angle)

        def rope(z):
            low, high = z[:, :head // 2], z[:, head // 2:]
            return jnp.concatenate([low * cos_t - high * sin_t, high * cos_t + low * sin_t], axis=1).astype(BF16).astype(F32)

        q0, q1, k = rope(q[:, :head]), rope(q[:, head:]), rope(k)
        groups = rows // 8

        def by_group(first, second):
            return jnp.concatenate([part8 for g in range(groups) for part8 in (first[8 * g:8 * g + 8], second[8 * g:8 * g + 8])], axis=0)

        q_all = by_group(q0, q1)
        s_new = jnp.sum(q_all * by_group(k, k), axis=1, keepdims=True)
        val_all = by_group(val, val)
        q_bf = q_all.astype(BF16)
        pos_all = by_group(pos, pos).astype(jnp.int32)
        for cp in kv_copies(c):
            cp.wait()

        def cached(i, g):
            return big[ff + 8 * ctx * g:ff + 8 * ctx * (g + 1), (2 * c + i) * head:(2 * c + i + 1) * head]

        for g in range(groups):
            sbuf[16 * g:16 * g + 16, :] = lax.dot_general(q_bf[16 * g:16 * g + 16], cached(0, g), (((1,), (1,)), ((), ())), preferred_element_type=F32)
        lane = lax.broadcasted_iota(jnp.int32, (2 * rows, 8 * ctx), 1)
        row = lax.broadcasted_iota(jnp.int32, (2 * rows, 8 * ctx), 0)
        valid = jnp.logical_and(lane // ctx == row % 8, lane % ctx < pos_all)
        s = ATTN_CAP * jnp.tanh(sbuf[:2 * rows, :] * (score_scale / ATTN_CAP))
        s_new = ATTN_CAP * jnp.tanh(s_new * (score_scale / ATTN_CAP))
        s = jnp.where(valid, s, -1e30)
        top = jnp.maximum(jnp.max(s, axis=1, keepdims=True), s_new)
        p = jnp.where(valid, jnp.exp(s - top), 0.0)
        p_new = jnp.exp(s_new - top)
        denom = jnp.sum(p, axis=1, keepdims=True) + p_new
        p_bf = p.astype(BF16)
        for g in range(groups):
            sbuf[16 * g:16 * g + 16, :head] = jnp.dot(p_bf[16 * g:16 * g + 16], cached(1, g), preferred_element_type=F32)
        o_all = (sbuf[:2 * rows, :head] + p_new.astype(BF16).astype(F32) * val_all) / denom
        o0 = jnp.concatenate([o_all[16 * g:16 * g + 8] for g in range(groups)], axis=0)
        o1 = jnp.concatenate([o_all[16 * g + 8:16 * g + 16] for g in range(groups)], axis=0)
        if c == 0:
            w_copies[3].wait()
        o = jnp.concatenate([o0, o1], axis=1).astype(BF16)
        part[c, :rows, :] = jnp.dot(o, wo[...], preferred_element_type=F32)
        if c + 1 == chunks:
            for cp in w_copies[5:]:
                cp.start()

    order = ((2, 1), (1, 2))

    def cols(h):
        return pl.ds(h * half, half)

    def rows_of(c, o):
        return pl.ds(pl.multiple_of(o * PIECES[c], 8), PIECES[c])

    def y_rows(c, o):
        return pl.ds(pl.multiple_of(group_rows(c) + o * PIECES[c], 8), PIECES[c])

    def remote(src, dst, c, phase, h, i, mask):
        return pltpu.make_async_remote_copy(src_ref=src, dst_ref=dst, send_sem=send_sem.at[c, phase, h, i], recv_sem=recv_sem.at[c, phase, h, i],
                                            device_id=(flip_t(t, mask), v), device_id_type=MESH)

    def scatter1(c, phase, h, i):
        m1, m2 = order[h]
        owner = flip_t(t, 3) if i else flip_t(t, m1)
        return remote(part.at[c, rows_of(c, owner), cols(h)], red1.at[c, h, i, pl.ds(0, PIECES[c])], c, phase, h, i, m1)

    def scatter2(c, phase, h):
        return remote(red1.at[c, h, 1, pl.ds(0, PIECES[c])], red2.at[c, h, pl.ds(0, PIECES[c])], c, phase, h, 2, order[h][1])

    def scatter_start(c, phase):
        for i in (1, 0):
            for h in range(2):
                scatter1(c, phase, h, i).start()

    def scatter_pass(c, phase):
        n = PIECES[c]
        for h in range(2):
            scatter1(c, phase, h, 1).wait_recv()
            red1[c, h, 1, :n] = red1[c, h, 1, :n] + part[c, rows_of(c, flip_t(t, order[h][1])), h * half:(h + 1) * half]
            scatter2(c, phase, h).start()

    def scatter_end(c, phase):
        n = PIECES[c]
        got = []
        for h in range(2):
            scatter1(c, phase, h, 0).wait_recv()
            scatter2(c, phase, h).wait_recv()
            got.append(part[c, rows_of(c, t), h * half:(h + 1) * half] + red1[c, h, 0, :n] + red2[c, h, :n])
        for h in range(2):
            scatter1(c, phase, h, 0).wait_send()
            scatter1(c, phase, h, 1).wait_send()
            scatter2(c, phase, h).wait_send()
        return jnp.concatenate(got, axis=1)

    def gather(c, h, i):
        m1, m2 = order[h]
        where = ybuf.at[y_rows(c, flip_t(t, m2) if i == 2 else t), cols(h)]
        return remote(where, where, c, 1, h, i, m1 if i else m2)

    def gather_start(c):
        for i in (0, 1):
            for h in range(2):
                gather(c, h, i).start()

    def gather_pass(c):
        for h in range(2):
            gather(c, h, 0).wait_recv()
            gather(c, h, 2).start()

    def gather_end(c):
        for h in range(2):
            gather(c, h, 1).wait_recv()
            gather(c, h, 2).wait_recv()
        for h in range(2):
            for i in range(3):
                gather(c, h, i).wait_send()

    def middle(c):
        attn_out = scatter_end(c, 0)
        x_own = xbuf[c, rows_of(c, t), :].astype(F32)
        x1 = (x_own + rms(attn_out, gain(g_attn_post))).astype(BF16).astype(F32)
        mid[c, :PIECES[c]] = x1
        ybuf[y_rows(c, t), :] = rms(x1, gain(g_mlp_pre)).astype(BF16).astype(F32)

    def mlp(c):
        rows = groups_of[c]
        gather_end(c)
        if c == 0:
            for cp in w_copies[4:]:
                cp.wait()
        m = ybuf[pl.ds(group_rows(c), rows), :].astype(BF16)
        tiles = 3
        wide = ff // tiles

        def up_tile(i, carry):
            at = pl.ds(pl.multiple_of(i * wide, 128), wide)
            gate = jnp.dot(m, big[:width, at], preferred_element_type=F32)
            up = jnp.dot(m, big[width:2 * width, at], preferred_element_type=F32)
            act[:rows, at] = (jax.nn.gelu(gate, approximate=True) * up).astype(BF16)
            return carry

        lax.fori_loop(0, tiles, up_tile, 0)

        def down_tile(i, carry):
            at = pl.ds(pl.multiple_of(i * wide, 128), wide)
            part[c, :rows, at] = jnp.dot(act[:rows, :], big[2 * width:2 * width + ff, at], preferred_element_type=F32)
            return carry

        lax.fori_loop(0, tiles, down_tile, 0)

    def finish(c):
        y = (mid[c, :PIECES[c]] + rms(scatter_end(c, 2), gain(g_mlp_post))).astype(BF16).astype(F32)
        ybuf[y_rows(c, t), :] = y
        spread(c, 0)

    def axes_of(p, bits):
        axes = [AXES[(p + s) % 3] for s in range(3)]
        mt = mv = 0
        for s in range(3):
            if bits >> s & 1:
                mt ^= FLIP[axes[s]][0]
                mv ^= FLIP[axes[s]][1]
        return mt, mv

    def block_copy(c, p, s, bits):
        mt, mv = axes_of(p, bits)
        blk = 4 * flip_v(v, mv) + flip_t(t, mt)
        at = ybuf.at[pl.ds(pl.multiple_of(bases[c] + blk * PIECES[c], 8), PIECES[c]), pl.ds(p * third, third)]
        ft, fv = FLIP['c'] if s == 3 else FLIP[AXES[(p + s) % 3]]
        i = 2 ** s - 1 + bits
        return pltpu.make_async_remote_copy(src_ref=at, dst_ref=at, send_sem=spread_send.at[c, p, i], recv_sem=spread_recv.at[c, p, i],
                                            device_id=(flip_t(t, ft), flip_v(v, fv)), device_id_type=MESH)

    def spread(c, step):
        if step == 0:
            for s in (0, 1, 2, 3):
                for p in range(3):
                    block_copy(c, p, s, 0).start()
        elif step <= 3:
            s = step - 1
            for bits in range(2 ** s):
                for p in range(3):
                    block_copy(c, p, s, bits).wait_recv()
                    for later in range(s + 1, 4):
                        block_copy(c, p, later, bits | 1 << s).start()
        else:
            for p in range(3):
                for bits in range(8):
                    block_copy(c, p, 3, bits).wait_recv()

    def spread_sent(c):
        for p in range(3):
            for s in range(4):
                for bits in range(2 ** s):
                    block_copy(c, p, s, bits).wait_send()

    sub = E_ROWS // 4
    vocab_local = e_hbm.shape[0]
    tiles = vocab_local // E_ROWS
    total = tiles * chunks

    def e_copy(i):
        return pltpu.make_async_copy(e_hbm.at[pl.ds(pl.multiple_of(i % tiles * E_ROWS, E_ROWS), E_ROWS)],
                                     big.at[pl.ds(pl.multiple_of(i % E_SLOTS * E_ROWS, E_ROWS), E_ROWS)], e_sem.at[i % E_SLOTS])

    def y_copy(c):
        return pltpu.make_async_copy(wo.at[pl.ds(0, toks_of[c])], y_hbm.at[pl.ds(bases[c], toks_of[c])], y_sem.at[c])

    def stat_copy(c, j):
        other = (me + j) % 16
        return pltpu.make_async_remote_copy(src_ref=stat.at[c], dst_ref=stats.at[c, me], send_sem=stat_send.at[c, j - 1], recv_sem=stat_recv.at[c, j - 1],
                                            device_id=(other % 4, other // 4), device_id_type=MESH)

    def reduce_rows(lg, toks, tgt, first_row):
        rel = tgt - first_row
        sublane = lax.broadcasted_iota(jnp.int32, (8, toks), 0)
        s_acc = [jnp.zeros((8, toks), F32) for _ in range(2)]
        t_acc = [jnp.zeros((8, toks), F32) for _ in range(2)]
        for r in range(sub // 8):
            th = jnp.tanh(lg[8 * r:8 * r + 8, :toks] * (1.0 / FINAL_CAP))
            s_acc[r % 2] = s_acc[r % 2] + jnp.exp(th * FINAL_CAP)
            t_acc[r % 2] = t_acc[r % 2] + jnp.where(sublane == rel - 8 * r, th, 0.0)
        return s_acc[0] + s_acc[1], t_acc[0] + t_acc[1]

    def head_pass(c, tasks):
        toks = toks_of[c]
        strip = 128
        if c:
            y_copy(c - 1).wait()
        for r in range(toks // strip):
            yv = ybuf[bases[c] + r * strip:bases[c] + (r + 1) * strip, :]
            wo[r * strip:(r + 1) * strip, :] = yv.astype(BF16)
            wq[:, r * strip:(r + 1) * strip] = rms(yv, gain(g_final)).T.astype(BF16)
        y_copy(c).start()
        first = bases[c] // 128
        tgt = jnp.concatenate([tgt_ref[first + q:first + q + 1, :] for q in range(toks // 128)], axis=1)
        tgt = jnp.broadcast_to(tgt, (8, toks)) - me * vocab_local

        def step(i, carry):
            s_sum, t_sum = carry
            n = c * tiles + i
            slot = n % E_SLOTS * E_ROWS
            e_copy(n).wait()
            for j in range(4):
                now, before = (lg0, lg1) if j % 2 == 0 else (lg1, lg0)
                now[:, :toks] = jnp.dot(big[pl.ds(pl.multiple_of(slot + j * sub, sub), sub), :], wq[:, :toks], preferred_element_type=F32)
                s_part, t_part = reduce_rows(before, toks, tgt, i * E_ROWS + (j - 1) * sub)
                if j == 0:
                    s_part, t_part = jnp.where(i > 0, s_part, 0.0), jnp.where(i > 0, t_part, 0.0)
                s_sum, t_sum = s_sum + s_part, t_sum + t_part

            @pl.when(n + E_SLOTS < total)
            def _():
                e_copy(n + E_SLOTS).start()

            for at, task in tasks:
                @pl.when(i == at)
                def _(task=task):
                    task()

            return s_sum, t_sum

        zero = jnp.zeros((8, toks), F32)
        s_sum, t_sum = lax.fori_loop(0, tiles, step, (zero, zero))
        s_part, t_part = reduce_rows(lg1, toks, tgt, tiles * E_ROWS - sub)
        s_sum = jnp.sum(s_sum + s_part, axis=0, keepdims=True)
        t_sum = jnp.sum(t_sum + t_part, axis=0, keepdims=True)
        sublane = lax.broadcasted_iota(jnp.int32, (8, toks), 0)
        both = jnp.where(sublane == 0, s_sum, jnp.where(sublane == 1, t_sum, 0.0))
        stat[c, :, :toks] = both
        stats[c, me, :, :toks] = both
        for j in range(1, 16):
            stat_copy(c, j).start()

    def combine(c):
        for j in range(1, 16):
            stat_copy(c, j).wait_recv()
        tot = stats[c, 0]
        for b in range(1, 16):
            tot = tot + stats[c, b]
        lp = FINAL_CAP * tot[1:2, :] - jnp.log(tot[0:1, :])
        for q in range(toks_of[c] // 128):
            logp_ref[bases[c] // 128 + q:bases[c] // 128 + q + 1, :] = lp[:, 128 * q:128 * (q + 1)]

    attend(0)
    lg1[...] = jnp.zeros_like(lg1)
    pl.semaphore_wait(barrier, 15)
    scatter_start(0, 0)
    attend(1)
    scatter_pass(0, 0)
    scatter_start(1, 0)
    middle(0)
    gather_start(0)
    scatter_pass(1, 0)
    gather_pass(0)
    middle(1)
    gather_start(1)
    mlp(0)
    scatter_start(0, 2)
    scatter_pass(0, 2)
    gather_pass(1)
    finish(0)
    spread(0, 1)
    mlp(1)
    for i in range(E_SLOTS):
        e_copy(i).start()
    spread(0, 2)
    spread(0, 3)
    spread(0, 4)
    scatter_start(1, 2)
    head_pass(0, ((0, lambda: scatter_pass(1, 2)), (2, lambda: finish(1)), (3, lambda: spread(1, 1)), (5, lambda: spread(1, 2)), (7, lambda: spread(1, 3)), (9, lambda: spread(1, 4))))
    head_pass(1, ((2, lambda: combine(0)),))
    combine(1)
    for c in range(chunks):
        spread_sent(c)
        for j in range(1, 16):
            stat_copy(c, j).wait_send()
    y_copy(chunks - 1).wait()


def step_kernel(x, seq, tgt, freq, gains, w_q, w_k, w_v, w_o, w_gate, w_up, w_down, k_rows, v_rows, table):
    tokens, width = x.shape
    chunks = len(PIECES)
    top = max(PIECES)
    rows, toks = 4 * top, 16 * top
    head = w_k.shape[1]
    ctx = k_rows.shape[0] // tokens
    ff = w_gate.shape[1]
    vm = pl.BlockSpec(memory_space=pltpu.VMEM)
    hbm = pl.BlockSpec(memory_space=pl.ANY)
    dma = pltpu.SemaphoreType.DMA
    return pl.pallas_call(
        kernel,
        out_shape=(jax.ShapeDtypeStruct((tokens // 128, 128), F32), jax.ShapeDtypeStruct((tokens, width), BF16)),
        in_specs=[hbm] + [vm] * 8 + [hbm] * 10,
        out_specs=(vm, hbm),
        scratch_shapes=[
            pltpu.VMEM((chunks, rows, width), BF16),
            pltpu.VMEM(w_q.shape, BF16),
            pltpu.VMEM(w_k.shape, BF16),
            pltpu.VMEM(w_v.shape, BF16),
            pltpu.VMEM(w_o.shape, BF16),
            pltpu.VMEM((2 * width + ff, ff), BF16),
            pltpu.VMEM((2 * rows, 8 * ctx), F32),
            pltpu.VMEM((chunks, rows, width), F32),
            pltpu.VMEM((chunks, 2, 2, top, width // 2), F32),
            pltpu.VMEM((chunks, 2, top, width // 2), F32),
            pltpu.VMEM((tokens, width), F32),
            pltpu.VMEM((chunks, top, width), F32),
            pltpu.VMEM((rows, ff), BF16),
            pltpu.VMEM((E_ROWS // 4, toks), F32),
            pltpu.VMEM((E_ROWS // 4, toks), F32),
            pltpu.VMEM((chunks, 8, toks), F32),
            pltpu.VMEM((chunks, 16, 8, toks), F32),
            dma((chunks,)),
            dma((7,)),
            dma((chunks, 2)),
            dma((E_SLOTS,)),
            dma((chunks,)),
            dma((chunks, 3, 2, 3)),
            dma((chunks, 3, 2, 3)),
            dma((chunks, 3, 15)),
            dma((chunks, 3, 15)),
            dma((chunks, 15)),
            dma((chunks, 15)),
        ],
        compiler_params=pltpu.CompilerParams(collective_id=0, has_side_effects=True, vmem_limit_bytes=67_000_000),
        name='step',
    )(x, seq, tgt, freq, *gains, w_q, w_k, w_v, w_o, w_gate, w_up, w_down, k_rows, v_rows, table)


def solution(mesh):
    in_specs = (P(), P(), P(), P(), P(None, 't'), P(None, 't'), P(None, 't'), P('t', None), P(), P(), P(None, 't'), P(None, 't'), P('t', None), P(), P(), P(None, None, 't', None), P(None, None, 't', None), P(('v', 't'), None))

    def local_step(hidden_in, seq_lens, target, g_attn_pre, w_q, w_k, w_v, w_o, g_attn_post, g_mlp_pre, w_gate, w_up, w_down, g_mlp_post, g_final, k_cache, v_cache, embed_table):
        tokens = hidden_in.shape[0]
        ctx, _, head_dim = k_cache.shape[1:]
        freq = ROPE_BASE ** (-2.0 * np.arange(head_dim // 2, dtype=np.float32) / head_dim)
        logp, hidden_out = step_kernel(
            hidden_in, seq_lens.reshape(-1, 128), target.reshape(-1, 128), jnp.asarray(freq[None, :], F32),
            (g_attn_pre, g_attn_post, g_mlp_pre, g_mlp_post, g_final), w_q, w_k, w_v, w_o, w_gate, w_up, w_down,
            k_cache.reshape(tokens * ctx, head_dim), v_cache.reshape(tokens * ctx, head_dim), embed_table)
        return logp.reshape(tokens), hidden_out

    return jax.shard_map(local_step, mesh=mesh, in_specs=in_specs, out_specs=(P(), P()), check_vma=False)
```

```python
import jax
import jax.numpy as jnp
import numpy as np
from jax import lax
from jax.experimental import pallas as pl
from jax.experimental.pallas import tpu as pltpu
from jax.sharding import PartitionSpec as P

ATTN_CAP = 50.0
FINAL_CAP = 30.0
NORM_EPS = 1e-6
ROPE_BASE = 10000.0
MESH = pl.DeviceIdType.MESH
F32 = jnp.float32
BF16 = jnp.bfloat16

PIECES = (32, 32)
E_ROWS = 1600
E_SLOTS = 4
AXES = ('x', 'z', 'y')
FLIP = {'x': (0, 2), 'y': (1, 0), 'z': (2, 0), 'c': (0, 1)}


def flip_t(t, mask):
    if mask == 0:
        return t
    if mask == 1:
        return t + 1 - 2 * (t % 2)
    if mask == 2:
        return (t + 2) % 4
    return 3 - t


def flip_v(v, mask):
    return flip_t(v, mask)


def rms(values, gain):
    return values * lax.rsqrt(jnp.mean(values * values, axis=-1, keepdims=True) + NORM_EPS) * gain


def kernel(x_hbm, seq_ref, tgt_ref, freq_ref, g_attn_pre, g_attn_post, g_mlp_pre, g_mlp_post, g_final,
           wq_hbm, wk_hbm, wv_hbm, wo_hbm, wg_hbm, wu_hbm, wd_hbm, k_hbm, v_hbm, e_hbm, stats, y_hbm,
           xbuf, wq, wk, wv, wo, big, sbuf, part, red1, red2, ybuf, mid, act, lg0, lg1, stat,
           x_sem, w_sem, kv_sem, e_sem, y_sem, send_sem, recv_sem, spread_send, spread_recv, stat_send, stat_recv):
    t = lax.axis_index('t')
    v = lax.axis_index('v')
    me = 4 * v + t
    chunks = len(PIECES)
    bases = [16 * sum(PIECES[:c]) for c in range(chunks)]
    width = x_hbm.shape[1]
    half, third = width // 2, width // 3
    ff = wg_hbm.shape[1]
    head = wk.shape[1]
    ctx = k_hbm.shape[0] // x_hbm.shape[0]
    score_scale = head ** -0.5
    groups_of = [4 * n for n in PIECES]
    toks_of = [16 * n for n in PIECES]

    def gain(ref):
        return 1.0 + ref[...].astype(F32).reshape(1, width)

    def group_rows(c):
        return pl.multiple_of(bases[c] + groups_of[c] * v, 8)

    x_copies = [pltpu.make_async_copy(x_hbm.at[pl.ds(group_rows(c), groups_of[c])], xbuf.at[c, pl.ds(0, groups_of[c])], x_sem.at[c]) for c in range(chunks)]

    def kv_at(c, i):
        return pl.ds(ff, groups_of[c] * ctx), pl.ds((2 * c + i) * head, head)

    def kv_copies(c):
        rows = pl.ds(pl.multiple_of(group_rows(c) * ctx, 8 * ctx), groups_of[c] * ctx)
        return [pltpu.make_async_copy(src.at[rows], big.at[kv_at(c, i)], kv_sem.at[c, i]) for i, src in enumerate((k_hbm, v_hbm))]

    pairs = ((wq_hbm, wq), (wk_hbm, wk), (wv_hbm, wv), (wo_hbm, wo), (wg_hbm, big.at[pl.ds(0, width)]), (wu_hbm, big.at[pl.ds(width, width)]), (wd_hbm, big.at[pl.ds(2 * width, ff)]))
    w_copies = [pltpu.make_async_copy(src, dst, w_sem.at[i]) for i, (src, dst) in enumerate(pairs)]
    x_copies[0].start()
    for cp in w_copies[:3]:
        cp.start()
    for cp in kv_copies(0):
        cp.start()
    w_copies[3].start()
    for c in range(1, chunks):
        x_copies[c].start()
        for cp in kv_copies(c):
            cp.start()
    w_copies[4].start()

    barrier = pltpu.get_barrier_semaphore()
    for j in range(1, 16):
        other = (me + j) % 16
        pl.semaphore_signal(barrier, inc=1, device_id=(other % 4, other // 4), device_id_type=MESH)

    def attend(c):
        rows = groups_of[c]
        x_copies[c].wait()
        a = rms(xbuf[c, :rows, :].astype(F32), gain(g_attn_pre)).astype(BF16)
        if c == 0:
            for cp in w_copies[:3]:
                cp.wait()
        q = jnp.dot(a, wq[...], preferred_element_type=F32)
        k = jnp.dot(a, wk[...], preferred_element_type=F32)
        val = jnp.dot(a, wv[...], preferred_element_type=F32).astype(BF16).astype(F32)
        start = group_rows(c)
        seq_row = seq_ref[pl.ds(start // 128, 1), :]
        lane = lax.broadcasted_iota(jnp.int32, (rows, 128), 1)
        row = lax.broadcasted_iota(jnp.int32, (rows, 128), 0)
        pos = jnp.sum(jnp.where(lane == row + start % 128, seq_row.astype(F32), 0.0), axis=1, keepdims=True)
        angle = pos * freq_ref[...]
        cos_t, sin_t = jnp.cos(angle), jnp.sin(angle)

        def rope(z):
            low, high = z[:, :head // 2], z[:, head // 2:]
            return jnp.concatenate([low * cos_t - high * sin_t, high * cos_t + low * sin_t], axis=1).astype(BF16).astype(F32)

        q0, q1, k = rope(q[:, :head]), rope(q[:, head:]), rope(k)
        groups = rows // 8

        def by_group(first, second):
            return jnp.concatenate([part8 for g in range(groups) for part8 in (first[8 * g:8 * g + 8], second[8 * g:8 * g + 8])], axis=0)

        q_all = by_group(q0, q1)
        s_new = jnp.sum(q_all * by_group(k, k), axis=1, keepdims=True)
        val_all = by_group(val, val)
        q_bf = q_all.astype(BF16)
        pos_all = by_group(pos, pos).astype(jnp.int32)
        for cp in kv_copies(c):
            cp.wait()

        def cached(i, g):
            return big[ff + 8 * ctx * g:ff + 8 * ctx * (g + 1), (2 * c + i) * head:(2 * c + i + 1) * head]

        for g in range(groups):
            sbuf[16 * g:16 * g + 16, :] = lax.dot_general(q_bf[16 * g:16 * g + 16], cached(0, g), (((1,), (1,)), ((), ())), preferred_element_type=F32)
        lane = lax.broadcasted_iota(jnp.int32, (2 * rows, 8 * ctx), 1)
        row = lax.broadcasted_iota(jnp.int32, (2 * rows, 8 * ctx), 0)
        valid = jnp.logical_and(lane // ctx == row % 8, lane % ctx < pos_all)
        s = ATTN_CAP * jnp.tanh(sbuf[:2 * rows, :] * (score_scale / ATTN_CAP))
        s_new = ATTN_CAP * jnp.tanh(s_new * (score_scale / ATTN_CAP))
        s = jnp.where(valid, s, -1e30)
        top = jnp.maximum(jnp.max(s, axis=1, keepdims=True), s_new)
        p = jnp.where(valid, jnp.exp(s - top), 0.0)
        p_new = jnp.exp(s_new - top)
        denom = jnp.sum(p, axis=1, keepdims=True) + p_new
        p_bf = p.astype(BF16)
        for g in range(groups):
            sbuf[16 * g:16 * g + 16, :head] = jnp.dot(p_bf[16 * g:16 * g + 16], cached(1, g), preferred_element_type=F32)
        o_all = (sbuf[:2 * rows, :head] + p_new.astype(BF16).astype(F32) * val_all) / denom
        o0 = jnp.concatenate([o_all[16 * g:16 * g + 8] for g in range(groups)], axis=0)
        o1 = jnp.concatenate([o_all[16 * g + 8:16 * g + 16] for g in range(groups)], axis=0)
        if c == 0:
            w_copies[3].wait()
        o = jnp.concatenate([o0, o1], axis=1).astype(BF16)
        part[c, :rows, :] = jnp.dot(o, wo[...], preferred_element_type=F32)
        if c + 1 == chunks:
            for cp in w_copies[5:]:
                cp.start()

    order = ((2, 1), (1, 2))

    def cols(h):
        return pl.ds(h * half, half)

    def rows_of(c, o):
        return pl.ds(pl.multiple_of(o * PIECES[c], 8), PIECES[c])

    def y_rows(c, o):
        return pl.ds(pl.multiple_of(group_rows(c) + o * PIECES[c], 8), PIECES[c])

    def remote(src, dst, c, phase, h, i, mask):
        return pltpu.make_async_remote_copy(src_ref=src, dst_ref=dst, send_sem=send_sem.at[c, phase, h, i], recv_sem=recv_sem.at[c, phase, h, i],
                                            device_id=(flip_t(t, mask), v), device_id_type=MESH)

    def scatter1(c, phase, h, i):
        m1, m2 = order[h]
        owner = flip_t(t, 3) if i else flip_t(t, m1)
        return remote(part.at[c, rows_of(c, owner), cols(h)], red1.at[c, h, i, pl.ds(0, PIECES[c])], c, phase, h, i, m1)

    def scatter2(c, phase, h):
        return remote(red1.at[c, h, 1, pl.ds(0, PIECES[c])], red2.at[c, h, pl.ds(0, PIECES[c])], c, phase, h, 2, order[h][1])

    def scatter_start(c, phase, halves=(0, 1)):
        for i in (1, 0):
            for h in halves:
                scatter1(c, phase, h, i).start()

    def scatter_pass(c, phase):
        n = PIECES[c]
        for h in range(2):
            scatter1(c, phase, h, 1).wait_recv()
            red1[c, h, 1, :n] = red1[c, h, 1, :n] + part[c, rows_of(c, flip_t(t, order[h][1])), h * half:(h + 1) * half]
            scatter2(c, phase, h).start()

    def scatter_end(c, phase):
        n = PIECES[c]
        got = []
        for h in range(2):
            scatter1(c, phase, h, 0).wait_recv()
            scatter2(c, phase, h).wait_recv()
            got.append(part[c, rows_of(c, t), h * half:(h + 1) * half] + red1[c, h, 0, :n] + red2[c, h, :n])
        for h in range(2):
            scatter1(c, phase, h, 0).wait_send()
            scatter1(c, phase, h, 1).wait_send()
            scatter2(c, phase, h).wait_send()
        return jnp.concatenate(got, axis=1)

    def gather(c, h, i):
        m1, m2 = order[h]
        where = ybuf.at[y_rows(c, flip_t(t, m2) if i == 2 else t), cols(h)]
        return remote(where, where, c, 1, h, i, m1 if i else m2)

    def gather_start(c):
        for i in (0, 1):
            for h in range(2):
                gather(c, h, i).start()

    def gather_pass(c):
        for h in range(2):
            gather(c, h, 0).wait_recv()
            gather(c, h, 2).start()

    def gather_end(c):
        for h in range(2):
            gather(c, h, 1).wait_recv()
            gather(c, h, 2).wait_recv()
        for h in range(2):
            for i in range(3):
                gather(c, h, i).wait_send()

    def middle(c):
        attn_out = scatter_end(c, 0)
        x_own = xbuf[c, rows_of(c, t), :].astype(F32)
        x1 = (x_own + rms(attn_out, gain(g_attn_post))).astype(BF16).astype(F32)
        mid[c, :PIECES[c]] = x1
        ybuf[y_rows(c, t), :] = rms(x1, gain(g_mlp_pre)).astype(BF16).astype(F32)

    def mlp(c, send):
        rows = groups_of[c]
        gather_end(c)
        if c == 0:
            for cp in w_copies[4:]:
                cp.wait()
        m = ybuf[pl.ds(group_rows(c), rows), :].astype(BF16)
        tiles = 3
        wide = ff // tiles

        def up_tile(i, carry):
            at = pl.ds(pl.multiple_of(i * wide, 128), wide)
            gate = jnp.dot(m, big[:width, at], preferred_element_type=F32)
            up = jnp.dot(m, big[width:2 * width, at], preferred_element_type=F32)
            act[:rows, at] = (jax.nn.gelu(gate, approximate=True) * up).astype(BF16)
            return carry

        lax.fori_loop(0, tiles, up_tile, 0)

        for h in range(2):
            part[c, :rows, h * half:(h + 1) * half] = jnp.dot(act[:rows, :], big[2 * width:2 * width + ff, h * half:(h + 1) * half], preferred_element_type=F32)
            if send:
                scatter_start(c, 2, (h,))

    def finish(c):
        y = (mid[c, :PIECES[c]] + rms(scatter_end(c, 2), gain(g_mlp_post))).astype(BF16).astype(F32)
        ybuf[y_rows(c, t), :] = y
        spread(c, 0)

    def axes_of(p, bits):
        axes = [AXES[(p + s) % 3] for s in range(3)]
        mt = mv = 0
        for s in range(3):
            if bits >> s & 1:
                mt ^= FLIP[axes[s]][0]
                mv ^= FLIP[axes[s]][1]
        return mt, mv

    def block_copy(c, p, s, bits):
        mt, mv = axes_of(p, bits)
        blk = 4 * flip_v(v, mv) + flip_t(t, mt)
        at = ybuf.at[pl.ds(pl.multiple_of(bases[c] + blk * PIECES[c], 8), PIECES[c]), pl.ds(p * third, third)]
        ft, fv = FLIP['c'] if s == 3 else FLIP[AXES[(p + s) % 3]]
        i = 2 ** s - 1 + bits
        return pltpu.make_async_remote_copy(src_ref=at, dst_ref=at, send_sem=spread_send.at[c, p, i], recv_sem=spread_recv.at[c, p, i],
                                            device_id=(flip_t(t, ft), flip_v(v, fv)), device_id_type=MESH)

    def spread(c, step):
        if step == 0:
            for s in (0, 1, 2, 3):
                for p in range(3):
                    block_copy(c, p, s, 0).start()
        elif step <= 3:
            s = step - 1
            for bits in range(2 ** s):
                for p in range(3):
                    block_copy(c, p, s, bits).wait_recv()
                    for later in range(s + 1, 4):
                        block_copy(c, p, later, bits | 1 << s).start()
        else:
            for p in range(3):
                for bits in range(8):
                    block_copy(c, p, 3, bits).wait_recv()

    def spread_sent(c):
        for p in range(3):
            for s in range(4):
                for bits in range(2 ** s):
                    block_copy(c, p, s, bits).wait_send()

    sub = E_ROWS // 4
    vocab_local = e_hbm.shape[0]
    tiles = vocab_local // E_ROWS
    total = tiles * chunks

    def e_copy(i):
        return pltpu.make_async_copy(e_hbm.at[pl.ds(pl.multiple_of(i % tiles * E_ROWS, E_ROWS), E_ROWS)],
                                     big.at[pl.ds(pl.multiple_of(i % E_SLOTS * E_ROWS, E_ROWS), E_ROWS)], e_sem.at[i % E_SLOTS])

    def y_copy(c):
        return pltpu.make_async_copy(wo.at[pl.ds(0, toks_of[c])], y_hbm.at[pl.ds(bases[c], toks_of[c])], y_sem.at[c])

    def stat_copy(c, j):
        other = (me + j) % 16
        return pltpu.make_async_remote_copy(src_ref=stat.at[c], dst_ref=stats.at[c, me], send_sem=stat_send.at[c, j - 1], recv_sem=stat_recv.at[c, j - 1],
                                            device_id=(other % 4, other // 4), device_id_type=MESH)

    def reduce_rows(lg, toks, tgt, first_row):
        rel = tgt - first_row
        sublane = lax.broadcasted_iota(jnp.int32, (8, toks), 0)
        s_acc = [jnp.zeros((8, toks), F32) for _ in range(2)]
        t_acc = [jnp.zeros((8, toks), F32) for _ in range(2)]
        for r in range(sub // 8):
            th = jnp.tanh(lg[8 * r:8 * r + 8, :toks] * (1.0 / FINAL_CAP))
            s_acc[r % 2] = s_acc[r % 2] + jnp.exp(th * FINAL_CAP)
            t_acc[r % 2] = t_acc[r % 2] + jnp.where(sublane == rel - 8 * r, th, 0.0)
        return s_acc[0] + s_acc[1], t_acc[0] + t_acc[1]

    def head_pass(c, per, tasks):
        toks = toks_of[c]
        strip = 128
        if c:
            y_copy(c - 1).wait()
        for r in range(toks // strip):
            yv = ybuf[bases[c] + r * strip:bases[c] + (r + 1) * strip, :]
            wo[r * strip:(r + 1) * strip, :] = yv.astype(BF16)
            wq[:, r * strip:(r + 1) * strip] = rms(yv, gain(g_final)).astype(BF16).T
        y_copy(c).start()
        first = bases[c] // 128
        tgt = jnp.concatenate([tgt_ref[first + q:first + q + 1, :] for q in range(toks // 128)], axis=1)
        tgt = jnp.broadcast_to(tgt, (8, toks)) - me * vocab_local

        def step(i, carry):
            s_sum, t_sum = carry
            n = c * tiles + i * per
            for k in range(per):
                e_copy(n + k).wait()
            for j in range(4 * per):
                now, before = (lg0, lg1) if j % 2 == 0 else (lg1, lg0)
                at = (n + j // 4) % E_SLOTS * E_ROWS + j % 4 * sub
                now[:, :toks] = jnp.dot(big[pl.ds(pl.multiple_of(at, sub), sub), :], wq[:, :toks], preferred_element_type=F32)
                s_part, t_part = reduce_rows(before, toks, tgt, i * per * E_ROWS + (j - 1) * sub)
                if j == 0:
                    s_part, t_part = jnp.where(i > 0, s_part, 0.0), jnp.where(i > 0, t_part, 0.0)
                s_sum, t_sum = s_sum + s_part, t_sum + t_part

            for k in range(per):
                @pl.when(n + k + E_SLOTS < total)
                def _(k=k):
                    e_copy(n + k + E_SLOTS).start()

            for at, task in tasks:
                @pl.when(i == at)
                def _(task=task):
                    task()

            return s_sum, t_sum

        zero = jnp.zeros((8, toks), F32)
        s_sum, t_sum = lax.fori_loop(0, tiles // per, step, (zero, zero))
        s_part, t_part = reduce_rows(lg1, toks, tgt, tiles * E_ROWS - sub)
        s_sum = jnp.sum(s_sum + s_part, axis=0, keepdims=True)
        t_sum = jnp.sum(t_sum + t_part, axis=0, keepdims=True)
        rows8 = [z[:, 128 * q:128 * (q + 1)] for z in (s_sum, t_sum) for q in range(toks // 128)]
        both = jnp.concatenate(rows8, axis=0)
        stat[c] = both
        stats[c, me] = both
        for j in range(1, 16):
            stat_copy(c, j).start()

    attend(0)
    lg1[...] = jnp.zeros_like(lg1)
    pl.semaphore_wait(barrier, 15)
    scatter_start(0, 0)
    attend(1)
    scatter_pass(0, 0)
    scatter_start(1, 0)
    middle(0)
    gather_start(0)
    scatter_pass(1, 0)
    gather_pass(0)
    middle(1)
    gather_start(1)
    mlp(0, True)
    scatter_pass(0, 2)
    gather_pass(1)
    finish(0)
    spread(0, 1)
    mlp(1, False)
    for i in range(E_SLOTS):
        e_copy(i).start()
    spread(0, 2)
    spread(0, 3)
    spread(0, 4)
    scatter_start(1, 2)
    head_pass(0, 1, ((0, lambda: scatter_pass(1, 2)), (2, lambda: finish(1)), (3, lambda: spread(1, 1)), (5, lambda: spread(1, 2)), (7, lambda: spread(1, 3)), (9, lambda: spread(1, 4))))
    head_pass(1, 2, ())
    for c in range(chunks):
        spread_sent(c)
        for j in range(1, 16):
            stat_copy(c, j).wait_recv()
            stat_copy(c, j).wait_send()
    y_copy(chunks - 1).wait()


def out_kernel(stats_hbm, y_hbm, logp_hbm, out_hbm, stats, logp, ybuf, stat_sem, in_sem, out_sem):
    pieces = in_sem.shape[0]
    n = ybuf.shape[0] // pieces
    get = pltpu.make_async_copy(stats_hbm, stats, stat_sem.at[0])
    get.start()

    def y_in(i):
        return pltpu.make_async_copy(y_hbm.at[pl.ds(i * n, n)], ybuf.at[pl.ds(i * n, n)], in_sem.at[i])

    def y_out(i):
        return pltpu.make_async_copy(ybuf.at[pl.ds(i * n, n)], out_hbm.at[pl.ds(i * n, n)], out_sem.at[i])

    for i in range(pieces):
        y_in(i).start()
    get.wait()
    first = 0
    for c, piece in enumerate(PIECES):
        tot = stats[c, 0]
        for b in range(1, stats.shape[1]):
            tot = tot + stats[c, b]
        rows = piece * 16 // 128
        logp[first:first + rows, :] = FINAL_CAP * tot[rows:2 * rows] - jnp.log(tot[:rows])
        first += rows
    put = pltpu.make_async_copy(logp, logp_hbm, stat_sem.at[1])
    put.start()
    for i in range(pieces):
        y_in(i).wait()
        y_out(i).start()
    put.wait()
    for i in range(pieces):
        y_out(i).wait()


def collect(stats, y):
    hbm = pl.BlockSpec(memory_space=pl.ANY)
    dma = pltpu.SemaphoreType.DMA
    return pl.pallas_call(
        out_kernel,
        out_shape=(jax.ShapeDtypeStruct((y.shape[0] // 128, 128), F32), jax.ShapeDtypeStruct(y.shape, y.dtype)),
        in_specs=[hbm, hbm],
        out_specs=(hbm, hbm),
        scratch_shapes=[pltpu.VMEM(stats.shape, F32), pltpu.VMEM((y.shape[0] // 128, 128), F32), pltpu.VMEM(y.shape, y.dtype), dma((2,)), dma((8,)), dma((8,))],
        name='collect',
    )(stats, y)


def step_kernel(x, seq, tgt, freq, gains, w_q, w_k, w_v, w_o, w_gate, w_up, w_down, k_rows, v_rows, table):
    tokens, width = x.shape
    chunks = len(PIECES)
    top = max(PIECES)
    rows, toks = 4 * top, 16 * top
    head = w_k.shape[1]
    ctx = k_rows.shape[0] // tokens
    ff = w_gate.shape[1]
    vm = pl.BlockSpec(memory_space=pltpu.VMEM)
    hbm = pl.BlockSpec(memory_space=pl.ANY)
    dma = pltpu.SemaphoreType.DMA
    return pl.pallas_call(
        kernel,
        out_shape=(jax.ShapeDtypeStruct((chunks, 16, 8, 128), F32), jax.ShapeDtypeStruct((tokens, width), BF16)),
        in_specs=[hbm] + [vm] * 8 + [hbm] * 10,
        out_specs=(vm, hbm),
        scratch_shapes=[
            pltpu.VMEM((chunks, rows, width), BF16),
            pltpu.VMEM(w_q.shape, BF16),
            pltpu.VMEM(w_k.shape, BF16),
            pltpu.VMEM(w_v.shape, BF16),
            pltpu.VMEM(w_o.shape, BF16),
            pltpu.VMEM((2 * width + ff, ff), BF16),
            pltpu.VMEM((2 * rows, 8 * ctx), F32),
            pltpu.VMEM((chunks, rows, width), F32),
            pltpu.VMEM((chunks, 2, 2, top, width // 2), F32),
            pltpu.VMEM((chunks, 2, top, width // 2), F32),
            pltpu.VMEM((tokens, width), F32),
            pltpu.VMEM((chunks, top, width), F32),
            pltpu.VMEM((rows, ff), BF16),
            pltpu.VMEM((E_ROWS // 4, toks), F32),
            pltpu.VMEM((E_ROWS // 4, toks), F32),
            pltpu.VMEM((chunks, 8, 128), F32),
            dma((chunks,)),
            dma((7,)),
            dma((chunks, 2)),
            dma((E_SLOTS,)),
            dma((chunks,)),
            dma((chunks, 3, 2, 3)),
            dma((chunks, 3, 2, 3)),
            dma((chunks, 3, 15)),
            dma((chunks, 3, 15)),
            dma((chunks, 15)),
            dma((chunks, 15)),
        ],
        compiler_params=pltpu.CompilerParams(collective_id=0, has_side_effects=True, vmem_limit_bytes=67_000_000),
        name='step',
    )(x, seq, tgt, freq, *gains, w_q, w_k, w_v, w_o, w_gate, w_up, w_down, k_rows, v_rows, table)


def solution(mesh):
    in_specs = (P(), P(), P(), P(), P(None, 't'), P(None, 't'), P(None, 't'), P('t', None), P(), P(), P(None, 't'), P(None, 't'), P('t', None), P(), P(), P(None, None, 't', None), P(None, None, 't', None), P(('v', 't'), None))

    def local_step(hidden_in, seq_lens, target, g_attn_pre, w_q, w_k, w_v, w_o, g_attn_post, g_mlp_pre, w_gate, w_up, w_down, g_mlp_post, g_final, k_cache, v_cache, embed_table):
        tokens = hidden_in.shape[0]
        ctx, _, head_dim = k_cache.shape[1:]
        freq = ROPE_BASE ** (-2.0 * np.arange(head_dim // 2, dtype=np.float32) / head_dim)
        stats, y = step_kernel(
            hidden_in, seq_lens.reshape(-1, 128), target.reshape(-1, 128), jnp.asarray(freq[None, :], F32),
            (g_attn_pre, g_attn_post, g_mlp_pre, g_mlp_post, g_final), w_q, w_k, w_v, w_o, w_gate, w_up, w_down,
            k_cache.reshape(tokens * ctx, head_dim), v_cache.reshape(tokens * ctx, head_dim), embed_table)
        logp, hidden_out = collect(stats, y)
        return logp.reshape(tokens), hidden_out

    return jax.shard_map(local_step, mesh=mesh, in_specs=in_specs, out_specs=(P(), P()), check_vma=False)
```

```python
import jax
import jax.numpy as jnp
import numpy as np
from jax import lax
from jax.experimental import pallas as pl
from jax.experimental.pallas import tpu as pltpu
from jax.sharding import PartitionSpec as P

ATTN_CAP = 50.0
FINAL_CAP = 30.0
NORM_EPS = 1e-6
ROPE_BASE = 10000.0
MESH = pl.DeviceIdType.MESH
F32 = jnp.float32
BF16 = jnp.bfloat16

PIECES = (32, 32)
E_ROWS = 1600
E_SLOTS = 4
AXES = ('x', 'z', 'y')
FLIP = {'x': (0, 2), 'y': (1, 0), 'z': (2, 0), 'c': (0, 1)}


def flip_t(t, mask):
    if mask == 0:
        return t
    if mask == 1:
        return t + 1 - 2 * (t % 2)
    if mask == 2:
        return (t + 2) % 4
    return 3 - t


def flip_v(v, mask):
    return flip_t(v, mask)


def rms(values, gain):
    return values * lax.rsqrt(jnp.mean(values * values, axis=-1, keepdims=True) + NORM_EPS) * gain


def kernel(x_hbm, seq_ref, tgt_ref, freq_ref, g_attn_pre, g_attn_post, g_mlp_pre, g_mlp_post, g_final,
           wq_hbm, wk_hbm, wv_hbm, wo_hbm, wg_hbm, wu_hbm, wd_hbm, k_hbm, v_hbm, e_hbm, stats, y_hbm,
           xbuf, wq, wk, wv, wo, big, sbuf, part, red1, red2, ybuf, mid, act, lg0, lg1, stat,
           x_sem, w_sem, kv_sem, e_sem, y_sem, send_sem, recv_sem, spread_send, spread_recv, stat_send, stat_recv):
    t = lax.axis_index('t')
    v = lax.axis_index('v')
    me = 4 * v + t
    chunks = len(PIECES)
    bases = [16 * sum(PIECES[:c]) for c in range(chunks)]
    width = x_hbm.shape[1]
    half, third = width // 2, width // 3
    ff = wg_hbm.shape[1]
    head = wk.shape[1]
    ctx = k_hbm.shape[0] // x_hbm.shape[0]
    score_scale = head ** -0.5
    groups_of = [4 * n for n in PIECES]
    toks_of = [16 * n for n in PIECES]

    def gain(ref):
        return 1.0 + ref[...].astype(F32).reshape(1, width)

    def group_rows(c):
        return pl.multiple_of(bases[c] + groups_of[c] * v, 8)

    x_copies = [pltpu.make_async_copy(x_hbm.at[pl.ds(group_rows(c), groups_of[c])], xbuf.at[c, pl.ds(0, groups_of[c])], x_sem.at[c]) for c in range(chunks)]

    def kv_at(c, i):
        return pl.ds(ff, groups_of[c] * ctx), pl.ds((2 * c + i) * head, head)

    def kv_copies(c):
        rows = pl.ds(pl.multiple_of(group_rows(c) * ctx, 8 * ctx), groups_of[c] * ctx)
        return [pltpu.make_async_copy(src.at[rows], big.at[kv_at(c, i)], kv_sem.at[c, i]) for i, src in enumerate((k_hbm, v_hbm))]

    pairs = ((wq_hbm, wq), (wk_hbm, wk), (wv_hbm, wv), (wo_hbm, wo), (wg_hbm, big.at[pl.ds(0, width)]), (wu_hbm, big.at[pl.ds(width, width)]), (wd_hbm, big.at[pl.ds(2 * width, ff)]))
    w_copies = [pltpu.make_async_copy(src, dst, w_sem.at[i]) for i, (src, dst) in enumerate(pairs)]
    x_copies[0].start()
    for cp in w_copies[:3]:
        cp.start()
    for cp in kv_copies(0):
        cp.start()
    w_copies[3].start()
    for c in range(1, chunks):
        x_copies[c].start()
        for cp in kv_copies(c):
            cp.start()
    w_copies[4].start()

    barrier = pltpu.get_barrier_semaphore()
    for j in range(1, 16):
        other = (me + j) % 16
        pl.semaphore_signal(barrier, inc=1, device_id=(other % 4, other // 4), device_id_type=MESH)

    def attend(c):
        rows = groups_of[c]
        x_copies[c].wait()
        a = rms(xbuf[c, :rows, :].astype(F32), gain(g_attn_pre)).astype(BF16)
        if c == 0:
            for cp in w_copies[:3]:
                cp.wait()
        q = jnp.dot(a, wq[...], preferred_element_type=F32)
        k = jnp.dot(a, wk[...], preferred_element_type=F32)
        val = jnp.dot(a, wv[...], preferred_element_type=F32).astype(BF16).astype(F32)
        start = group_rows(c)
        seq_row = seq_ref[pl.ds(start // 128, 1), :]
        lane = lax.broadcasted_iota(jnp.int32, (rows, 128), 1)
        row = lax.broadcasted_iota(jnp.int32, (rows, 128), 0)
        pos = jnp.sum(jnp.where(lane == row + start % 128, seq_row.astype(F32), 0.0), axis=1, keepdims=True)
        angle = pos * freq_ref[...]
        cos_t, sin_t = jnp.cos(angle), jnp.sin(angle)

        def rope(z):
            low, high = z[:, :head // 2], z[:, head // 2:]
            return jnp.concatenate([low * cos_t - high * sin_t, high * cos_t + low * sin_t], axis=1).astype(BF16).astype(F32)

        q0, q1, k = rope(q[:, :head]), rope(q[:, head:]), rope(k)
        groups = rows // 8

        def by_group(first, second):
            return jnp.concatenate([part8 for g in range(groups) for part8 in (first[8 * g:8 * g + 8], second[8 * g:8 * g + 8])], axis=0)

        q_all = by_group(q0, q1)
        s_new = jnp.sum(q_all * by_group(k, k), axis=1, keepdims=True)
        val_all = by_group(val, val)
        q_bf = q_all.astype(BF16)
        pos_all = by_group(pos, pos).astype(jnp.int32)
        for cp in kv_copies(c):
            cp.wait()

        def cached(i, g):
            return big[ff + 8 * ctx * g:ff + 8 * ctx * (g + 1), (2 * c + i) * head:(2 * c + i + 1) * head]

        for g in range(groups):
            sbuf[16 * g:16 * g + 16, :] = lax.dot_general(q_bf[16 * g:16 * g + 16], cached(0, g), (((1,), (1,)), ((), ())), preferred_element_type=F32)
        lane = lax.broadcasted_iota(jnp.int32, (2 * rows, 8 * ctx), 1)
        row = lax.broadcasted_iota(jnp.int32, (2 * rows, 8 * ctx), 0)
        valid = jnp.logical_and(lane // ctx == row % 8, lane % ctx < pos_all)
        s = ATTN_CAP * jnp.tanh(sbuf[:2 * rows, :] * (score_scale / ATTN_CAP))
        s_new = ATTN_CAP * jnp.tanh(s_new * (score_scale / ATTN_CAP))
        s = jnp.where(valid, s, -1e30)
        top = jnp.maximum(jnp.max(s, axis=1, keepdims=True), s_new)
        p = jnp.where(valid, jnp.exp(s - top), 0.0)
        p_new = jnp.exp(s_new - top)
        denom = jnp.sum(p, axis=1, keepdims=True) + p_new
        p_bf = p.astype(BF16)
        for g in range(groups):
            sbuf[16 * g:16 * g + 16, :head] = jnp.dot(p_bf[16 * g:16 * g + 16], cached(1, g), preferred_element_type=F32)
        o_all = (sbuf[:2 * rows, :head] + p_new.astype(BF16).astype(F32) * val_all) / denom
        o0 = jnp.concatenate([o_all[16 * g:16 * g + 8] for g in range(groups)], axis=0)
        o1 = jnp.concatenate([o_all[16 * g + 8:16 * g + 16] for g in range(groups)], axis=0)
        if c == 0:
            w_copies[3].wait()
        o = jnp.concatenate([o0, o1], axis=1).astype(BF16)
        part[c, :rows, :] = jnp.dot(o, wo[...], preferred_element_type=F32)
        if c + 1 == chunks:
            for cp in w_copies[5:]:
                cp.start()

    order = ((2, 1), (1, 2))

    def cols(h):
        return pl.ds(h * half, half)

    def rows_of(c, o):
        return pl.ds(pl.multiple_of(o * PIECES[c], 8), PIECES[c])

    def y_rows(c, o):
        return pl.ds(pl.multiple_of(group_rows(c) + o * PIECES[c], 8), PIECES[c])

    def remote(src, dst, c, phase, h, i, mask):
        return pltpu.make_async_remote_copy(src_ref=src, dst_ref=dst, send_sem=send_sem.at[c, phase, h, i], recv_sem=recv_sem.at[c, phase, h, i],
                                            device_id=(flip_t(t, mask), v), device_id_type=MESH)

    def scatter1(c, phase, h, i):
        m1, m2 = order[h]
        owner = flip_t(t, 3) if i else flip_t(t, m1)
        return remote(part.at[c, rows_of(c, owner), cols(h)], red1.at[c, h, i, pl.ds(0, PIECES[c])], c, phase, h, i, m1)

    def scatter2(c, phase, h):
        return remote(red1.at[c, h, 1, pl.ds(0, PIECES[c])], red2.at[c, h, pl.ds(0, PIECES[c])], c, phase, h, 2, order[h][1])

    def scatter_start(c, phase, halves=(0, 1)):
        for i in (1, 0):
            for h in halves:
                scatter1(c, phase, h, i).start()

    def scatter_pass(c, phase):
        n = PIECES[c]
        for h in range(2):
            scatter1(c, phase, h, 1).wait_recv()
            red1[c, h, 1, :n] = red1[c, h, 1, :n] + part[c, rows_of(c, flip_t(t, order[h][1])), h * half:(h + 1) * half]
            scatter2(c, phase, h).start()

    def scatter_end(c, phase):
        n = PIECES[c]
        got = []
        for h in range(2):
            scatter1(c, phase, h, 0).wait_recv()
            scatter2(c, phase, h).wait_recv()
            got.append(part[c, rows_of(c, t), h * half:(h + 1) * half] + red1[c, h, 0, :n] + red2[c, h, :n])
        for h in range(2):
            scatter1(c, phase, h, 0).wait_send()
            scatter1(c, phase, h, 1).wait_send()
            scatter2(c, phase, h).wait_send()
        return jnp.concatenate(got, axis=1)

    def gather(c, h, i):
        m1, m2 = order[h]
        where = ybuf.at[y_rows(c, flip_t(t, m2) if i == 2 else t), cols(h)]
        return remote(where, where, c, 1, h, i, m1 if i else m2)

    def gather_start(c):
        for i in (0, 1):
            for h in range(2):
                gather(c, h, i).start()

    def gather_pass(c):
        for h in range(2):
            gather(c, h, 0).wait_recv()
            gather(c, h, 2).start()

    def gather_end(c):
        for h in range(2):
            gather(c, h, 1).wait_recv()
            gather(c, h, 2).wait_recv()
        for h in range(2):
            for i in range(3):
                gather(c, h, i).wait_send()

    def middle(c):
        attn_out = scatter_end(c, 0)
        x_own = xbuf[c, rows_of(c, t), :].astype(F32)
        x1 = (x_own + rms(attn_out, gain(g_attn_post))).astype(BF16).astype(F32)
        mid[c, :PIECES[c]] = x1
        ybuf[y_rows(c, t), :] = rms(x1, gain(g_mlp_pre)).astype(BF16).astype(F32)

    def mlp(c, send):
        rows = groups_of[c]
        gather_end(c)
        if c == 0:
            for cp in w_copies[4:]:
                cp.wait()
        m = ybuf[pl.ds(group_rows(c), rows), :].astype(BF16)
        tiles = 3
        wide = ff // tiles

        def up_tile(i, carry):
            at = pl.ds(pl.multiple_of(i * wide, 128), wide)
            gate = jnp.dot(m, big[:width, at], preferred_element_type=F32)
            up = jnp.dot(m, big[width:2 * width, at], preferred_element_type=F32)
            act[:rows, at] = (jax.nn.gelu(gate, approximate=True) * up).astype(BF16)
            return carry

        lax.fori_loop(0, tiles, up_tile, 0)

        for h in range(2):
            part[c, :rows, h * half:(h + 1) * half] = jnp.dot(act[:rows, :], big[2 * width:2 * width + ff, h * half:(h + 1) * half], preferred_element_type=F32)
            if send:
                scatter_start(c, 2, (h,))

    def finish(c):
        y = (mid[c, :PIECES[c]] + rms(scatter_end(c, 2), gain(g_mlp_post))).astype(BF16).astype(F32)
        ybuf[y_rows(c, t), :] = y
        spread(c, 0)

    def axes_of(p, bits):
        axes = [AXES[(p + s) % 3] for s in range(3)]
        mt = mv = 0
        for s in range(3):
            if bits >> s & 1:
                mt ^= FLIP[axes[s]][0]
                mv ^= FLIP[axes[s]][1]
        return mt, mv

    def block_copy(c, p, s, bits):
        mt, mv = axes_of(p, bits)
        blk = 4 * flip_v(v, mv) + flip_t(t, mt)
        at = ybuf.at[pl.ds(pl.multiple_of(bases[c] + blk * PIECES[c], 8), PIECES[c]), pl.ds(p * third, third)]
        ft, fv = FLIP['c'] if s == 3 else FLIP[AXES[(p + s) % 3]]
        i = 2 ** s - 1 + bits
        return pltpu.make_async_remote_copy(src_ref=at, dst_ref=at, send_sem=spread_send.at[c, p, i], recv_sem=spread_recv.at[c, p, i],
                                            device_id=(flip_t(t, ft), flip_v(v, fv)), device_id_type=MESH)

    def spread(c, step):
        if step == 0:
            for s in (0, 1, 2, 3):
                for p in range(3):
                    block_copy(c, p, s, 0).start()
        elif step <= 3:
            s = step - 1
            for bits in range(2 ** s):
                for p in range(3):
                    block_copy(c, p, s, bits).wait_recv()
                    for later in range(s + 1, 4):
                        block_copy(c, p, later, bits | 1 << s).start()
        else:
            for p in range(3):
                for bits in range(8):
                    block_copy(c, p, 3, bits).wait_recv()

    def spread_sent(c):
        for p in range(3):
            for s in range(4):
                for bits in range(2 ** s):
                    block_copy(c, p, s, bits).wait_send()

    sub = E_ROWS // 4
    vocab_local = e_hbm.shape[0]
    tiles = vocab_local // E_ROWS
    total = tiles * chunks

    def e_copy(i):
        return pltpu.make_async_copy(e_hbm.at[pl.ds(pl.multiple_of(i % tiles * E_ROWS, E_ROWS), E_ROWS)],
                                     big.at[pl.ds(pl.multiple_of(i % E_SLOTS * E_ROWS, E_ROWS), E_ROWS)], e_sem.at[i % E_SLOTS])

    def y_copy(c):
        return pltpu.make_async_copy(wo.at[pl.ds(0, toks_of[c])], y_hbm.at[pl.ds(bases[c], toks_of[c])], y_sem.at[c])

    def stat_copy(c, j):
        other = (me + j) % 16
        return pltpu.make_async_remote_copy(src_ref=stat.at[c], dst_ref=stats.at[c, me], send_sem=stat_send.at[c, j - 1], recv_sem=stat_recv.at[c, j - 1],
                                            device_id=(other % 4, other // 4), device_id_type=MESH)

    def own_stat(c):
        return pltpu.make_async_copy(stat.at[c], stats.at[c, me], y_sem.at[chunks + c])

    def reduce_rows(lg, toks, tgt, first_row):
        rel = tgt - first_row
        sublane = lax.broadcasted_iota(jnp.int32, (8, toks), 0)
        s_acc = [jnp.zeros((8, toks), F32) for _ in range(2)]
        t_acc = [jnp.zeros((8, toks), F32) for _ in range(2)]
        for r in range(sub // 8):
            th = jnp.tanh(lg[8 * r:8 * r + 8, :toks] * (1.0 / FINAL_CAP))
            s_acc[r % 2] = s_acc[r % 2] + jnp.exp(th * FINAL_CAP)
            t_acc[r % 2] = t_acc[r % 2] + jnp.where(sublane == rel - 8 * r, th, 0.0)
        return s_acc[0] + s_acc[1], t_acc[0] + t_acc[1]

    def head_pass(c, per, tasks):
        toks = toks_of[c]
        strip = 128
        if c:
            y_copy(c - 1).wait()
        for r in range(toks // strip):
            yv = ybuf[bases[c] + r * strip:bases[c] + (r + 1) * strip, :]
            wo[r * strip:(r + 1) * strip, :] = yv.astype(BF16)
            wq[:, r * strip:(r + 1) * strip] = rms(yv, gain(g_final)).astype(BF16).T
        y_copy(c).start()
        first = bases[c] // 128
        tgt = jnp.concatenate([tgt_ref[first + q:first + q + 1, :] for q in range(toks // 128)], axis=1)
        tgt = jnp.broadcast_to(tgt, (8, toks)) - me * vocab_local

        def step(i, carry):
            s_sum, t_sum = carry
            n = c * tiles + i * per
            for k in range(per):
                e_copy(n + k).wait()
            for j in range(4 * per):
                now, before = (lg0, lg1) if j % 2 == 0 else (lg1, lg0)
                at = (n + j // 4) % E_SLOTS * E_ROWS + j % 4 * sub
                now[:, :toks] = jnp.dot(big[pl.ds(pl.multiple_of(at, sub), sub), :], wq[:, :toks], preferred_element_type=F32)
                s_part, t_part = reduce_rows(before, toks, tgt, i * per * E_ROWS + (j - 1) * sub)
                if j == 0:
                    s_part, t_part = jnp.where(i > 0, s_part, 0.0), jnp.where(i > 0, t_part, 0.0)
                s_sum, t_sum = s_sum + s_part, t_sum + t_part

            for k in range(per):
                @pl.when(n + k + E_SLOTS < total)
                def _(k=k):
                    e_copy(n + k + E_SLOTS).start()

            for at, task in tasks:
                @pl.when(i == at)
                def _(task=task):
                    task()

            return s_sum, t_sum

        zero = jnp.zeros((8, toks), F32)
        s_sum, t_sum = lax.fori_loop(0, tiles // per, step, (zero, zero))
        s_part, t_part = reduce_rows(lg1, toks, tgt, tiles * E_ROWS - sub)
        s_sum = jnp.sum(s_sum + s_part, axis=0, keepdims=True)
        t_sum = jnp.sum(t_sum + t_part, axis=0, keepdims=True)
        rows8 = [z[:, 128 * q:128 * (q + 1)] for z in (s_sum, t_sum) for q in range(toks // 128)]
        both = jnp.concatenate(rows8, axis=0)
        stat[c] = both
        own_stat(c).start()
        for j in range(1, 16):
            stat_copy(c, j).start()

    attend(0)
    lg1[...] = jnp.zeros_like(lg1)
    pl.semaphore_wait(barrier, 15)
    scatter_start(0, 0)
    attend(1)
    scatter_pass(0, 0)
    scatter_start(1, 0)
    middle(0)
    gather_start(0)
    scatter_pass(1, 0)
    gather_pass(0)
    middle(1)
    gather_start(1)
    mlp(0, True)
    scatter_pass(0, 2)
    gather_pass(1)
    finish(0)
    spread(0, 1)
    mlp(1, False)
    for i in range(E_SLOTS):
        e_copy(i).start()
    spread(0, 2)
    scatter_start(1, 2)
    spread(0, 3)
    spread(0, 4)
    head_pass(0, 1, ((0, lambda: scatter_pass(1, 2)), (2, lambda: finish(1)), (4, lambda: spread(1, 1)), (6, lambda: spread(1, 2)), (8, lambda: spread(1, 3)), (9, lambda: spread(1, 4))))
    head_pass(1, 2, ())
    for c in range(chunks):
        spread_sent(c)
        own_stat(c).wait()
        for j in range(1, 16):
            stat_copy(c, j).wait_recv()
            stat_copy(c, j).wait_send()
    y_copy(chunks - 1).wait()


def out_kernel(stats_hbm, y_hbm, logp_hbm, out_hbm, stats, logp, ybuf, stat_sem, in_sem, out_sem):
    pieces = in_sem.shape[0]
    n = ybuf.shape[0] // pieces
    get = pltpu.make_async_copy(stats_hbm, stats, stat_sem.at[0])
    get.start()

    def y_in(i):
        return pltpu.make_async_copy(y_hbm.at[pl.ds(i * n, n)], ybuf.at[pl.ds(i * n, n)], in_sem.at[i])

    def y_out(i):
        return pltpu.make_async_copy(ybuf.at[pl.ds(i * n, n)], out_hbm.at[pl.ds(i * n, n)], out_sem.at[i])

    for i in range(pieces):
        y_in(i).start()
    get.wait()
    first = 0
    for c, piece in enumerate(PIECES):
        tot = stats[c, 0]
        for b in range(1, stats.shape[1]):
            tot = tot + stats[c, b]
        rows = piece * 16 // 128
        logp[first:first + rows, :] = FINAL_CAP * tot[rows:2 * rows] - jnp.log(tot[:rows])
        first += rows
    put = pltpu.make_async_copy(logp, logp_hbm, stat_sem.at[1])
    put.start()
    for i in range(pieces):
        y_in(i).wait()
        y_out(i).start()
    put.wait()
    for i in range(pieces):
        y_out(i).wait()


def collect(stats, y):
    hbm = pl.BlockSpec(memory_space=pl.ANY)
    dma = pltpu.SemaphoreType.DMA
    return pl.pallas_call(
        out_kernel,
        out_shape=(jax.ShapeDtypeStruct((y.shape[0] // 128, 128), F32), jax.ShapeDtypeStruct(y.shape, y.dtype)),
        in_specs=[hbm, hbm],
        out_specs=(hbm, hbm),
        scratch_shapes=[pltpu.VMEM(stats.shape, F32), pltpu.VMEM((y.shape[0] // 128, 128), F32), pltpu.VMEM(y.shape, y.dtype), dma((2,)), dma((8,)), dma((8,))],
        name='collect',
    )(stats, y)


def step_kernel(x, seq, tgt, freq, gains, w_q, w_k, w_v, w_o, w_gate, w_up, w_down, k_rows, v_rows, table):
    tokens, width = x.shape
    chunks = len(PIECES)
    top = max(PIECES)
    rows, toks = 4 * top, 16 * top
    head = w_k.shape[1]
    ctx = k_rows.shape[0] // tokens
    ff = w_gate.shape[1]
    vm = pl.BlockSpec(memory_space=pltpu.VMEM)
    hbm = pl.BlockSpec(memory_space=pl.ANY)
    dma = pltpu.SemaphoreType.DMA
    return pl.pallas_call(
        kernel,
        out_shape=(jax.ShapeDtypeStruct((chunks, 16, 8, 128), F32), jax.ShapeDtypeStruct((tokens, width), BF16)),
        in_specs=[hbm] + [vm] * 8 + [hbm] * 10,
        out_specs=(hbm, hbm),
        scratch_shapes=[
            pltpu.VMEM((chunks, rows, width), BF16),
            pltpu.VMEM(w_q.shape, BF16),
            pltpu.VMEM(w_k.shape, BF16),
            pltpu.VMEM(w_v.shape, BF16),
            pltpu.VMEM(w_o.shape, BF16),
            pltpu.VMEM((2 * width + ff, ff), BF16),
            pltpu.VMEM((2 * rows, 8 * ctx), F32),
            pltpu.VMEM((chunks, rows, width), F32),
            pltpu.VMEM((chunks, 2, 2, top, width // 2), F32),
            pltpu.VMEM((chunks, 2, top, width // 2), F32),
            pltpu.VMEM((tokens, width), F32),
            pltpu.VMEM((chunks, top, width), F32),
            pltpu.VMEM((rows, ff), BF16),
            pltpu.VMEM((E_ROWS // 4, toks), F32),
            pltpu.VMEM((E_ROWS // 4, toks), F32),
            pltpu.VMEM((chunks, 8, 128), F32),
            dma((chunks,)),
            dma((7,)),
            dma((chunks, 2)),
            dma((E_SLOTS,)),
            dma((2 * chunks,)),
            dma((chunks, 3, 2, 3)),
            dma((chunks, 3, 2, 3)),
            dma((chunks, 3, 15)),
            dma((chunks, 3, 15)),
            dma((chunks, 15)),
            dma((chunks, 15)),
        ],
        compiler_params=pltpu.CompilerParams(collective_id=0, has_side_effects=True, vmem_limit_bytes=67_000_000),
        name='step',
    )(x, seq, tgt, freq, *gains, w_q, w_k, w_v, w_o, w_gate, w_up, w_down, k_rows, v_rows, table)


def solution(mesh):
    in_specs = (P(), P(), P(), P(), P(None, 't'), P(None, 't'), P(None, 't'), P('t', None), P(), P(), P(None, 't'), P(None, 't'), P('t', None), P(), P(), P(None, None, 't', None), P(None, None, 't', None), P(('v', 't'), None))

    def local_step(hidden_in, seq_lens, target, g_attn_pre, w_q, w_k, w_v, w_o, g_attn_post, g_mlp_pre, w_gate, w_up, w_down, g_mlp_post, g_final, k_cache, v_cache, embed_table):
        tokens = hidden_in.shape[0]
        ctx, _, head_dim = k_cache.shape[1:]
        freq = ROPE_BASE ** (-2.0 * np.arange(head_dim // 2, dtype=np.float32) / head_dim)
        stats, y = step_kernel(
            hidden_in, seq_lens.reshape(-1, 128), target.reshape(-1, 128), jnp.asarray(freq[None, :], F32),
            (g_attn_pre, g_attn_post, g_mlp_pre, g_mlp_post, g_final), w_q, w_k, w_v, w_o, w_gate, w_up, w_down,
            k_cache.reshape(tokens * ctx, head_dim), v_cache.reshape(tokens * ctx, head_dim), embed_table)
        logp, hidden_out = collect(stats, y)
        return logp.reshape(tokens), hidden_out

    return jax.shard_map(local_step, mesh=mesh, in_specs=in_specs, out_specs=(P(), P()), check_vma=False)
```

```python
import jax
import jax.numpy as jnp
import numpy as np
from jax import lax
from jax.experimental import pallas as pl
from jax.experimental.pallas import tpu as pltpu
from jax.sharding import PartitionSpec as P

ATTN_CAP = 50.0
FINAL_CAP = 30.0
NORM_EPS = 1e-6
ROPE_BASE = 10000.0
MESH = pl.DeviceIdType.MESH
F32 = jnp.float32
BF16 = jnp.bfloat16

PIECES = (32, 32)
E_ROWS = 1600
E_SLOTS = 4
AXES = ('x', 'z', 'y')
FLIP = {'x': (0, 2), 'y': (1, 0), 'z': (2, 0), 'c': (0, 1)}


def flip_t(t, mask):
    if mask == 0:
        return t
    if mask == 1:
        return t + 1 - 2 * (t % 2)
    if mask == 2:
        return (t + 2) % 4
    return 3 - t


def flip_v(v, mask):
    return flip_t(v, mask)


def rms(values, gain):
    return values * lax.rsqrt(jnp.mean(values * values, axis=-1, keepdims=True) + NORM_EPS) * gain


def kernel(x_hbm, seq_ref, tgt_ref, freq_ref, g_attn_pre, g_attn_post, g_mlp_pre, g_mlp_post, g_final,
           wq_hbm, wk_hbm, wv_hbm, wo_hbm, wg_hbm, wu_hbm, wd_hbm, k_hbm, v_hbm, e_hbm, stats, y_hbm,
           xbuf, wq, wk, wv, wo, big, sbuf, part, red1, red2, ybuf, mid, act, lg0, lg1, stat,
           x_sem, w_sem, kv_sem, e_sem, y_sem, send_sem, recv_sem, spread_send, spread_recv, stat_send, stat_recv):
    t = lax.axis_index('t')
    v = lax.axis_index('v')
    me = 4 * v + t
    chunks = len(PIECES)
    bases = [16 * sum(PIECES[:c]) for c in range(chunks)]
    width = x_hbm.shape[1]
    half, third = width // 2, width // 3
    ff = wg_hbm.shape[1]
    head = wk.shape[1]
    ctx = k_hbm.shape[0] // x_hbm.shape[0]
    score_scale = head ** -0.5
    groups_of = [4 * n for n in PIECES]
    toks_of = [16 * n for n in PIECES]

    def gain(ref):
        return 1.0 + ref[...].astype(F32).reshape(1, width)

    def group_rows(c):
        return pl.multiple_of(bases[c] + groups_of[c] * v, 8)

    x_copies = [pltpu.make_async_copy(x_hbm.at[pl.ds(group_rows(c), groups_of[c])], xbuf.at[c, pl.ds(0, groups_of[c])], x_sem.at[c]) for c in range(chunks)]

    def kv_at(c, i):
        return pl.ds(ff, groups_of[c] * ctx), pl.ds((2 * c + i) * head, head)

    def kv_copies(c):
        rows = pl.ds(pl.multiple_of(group_rows(c) * ctx, 8 * ctx), groups_of[c] * ctx)
        return [pltpu.make_async_copy(src.at[rows], big.at[kv_at(c, i)], kv_sem.at[c, i]) for i, src in enumerate((k_hbm, v_hbm))]

    pairs = ((wq_hbm, wq), (wk_hbm, wk), (wv_hbm, wv), (wo_hbm, wo), (wg_hbm, big.at[pl.ds(0, width)]), (wu_hbm, big.at[pl.ds(width, width)]), (wd_hbm, big.at[pl.ds(2 * width, ff)]))
    w_copies = [pltpu.make_async_copy(src, dst, w_sem.at[i]) for i, (src, dst) in enumerate(pairs)]
    x_copies[0].start()
    for cp in w_copies[:3]:
        cp.start()

    barrier = pltpu.get_barrier_semaphore()
    for j in range(1, 16):
        other = (me + j) % 16
        pl.semaphore_signal(barrier, inc=1, device_id=(other % 4, other // 4), device_id_type=MESH)

    def attend(c):
        rows = groups_of[c]
        x_copies[c].wait()
        if c == 0:
            for cp in kv_copies(0):
                cp.start()
        a = rms(xbuf[c, :rows, :].astype(F32), gain(g_attn_pre)).astype(BF16)
        if c == 0:
            for cp in w_copies[:3]:
                cp.wait()
            w_copies[3].start()
            for later in range(1, chunks):
                x_copies[later].start()
                for cp in kv_copies(later):
                    cp.start()
        q = jnp.dot(a, wq[...], preferred_element_type=F32)
        k = jnp.dot(a, wk[...], preferred_element_type=F32)
        val = jnp.dot(a, wv[...], preferred_element_type=F32).astype(BF16).astype(F32)
        start = group_rows(c)
        seq_row = seq_ref[pl.ds(start // 128, 1), :]
        lane = lax.broadcasted_iota(jnp.int32, (rows, 128), 1)
        row = lax.broadcasted_iota(jnp.int32, (rows, 128), 0)
        pos = jnp.sum(jnp.where(lane == row + start % 128, seq_row.astype(F32), 0.0), axis=1, keepdims=True)
        angle = pos * freq_ref[...]
        cos_t, sin_t = jnp.cos(angle), jnp.sin(angle)

        def rope(z):
            low, high = z[:, :head // 2], z[:, head // 2:]
            return jnp.concatenate([low * cos_t - high * sin_t, high * cos_t + low * sin_t], axis=1).astype(BF16).astype(F32)

        q0, q1, k = rope(q[:, :head]), rope(q[:, head:]), rope(k)
        groups = rows // 8

        def by_group(first, second):
            return jnp.concatenate([part8 for g in range(groups) for part8 in (first[8 * g:8 * g + 8], second[8 * g:8 * g + 8])], axis=0)

        q_all = by_group(q0, q1)
        s_new = jnp.sum(q_all * by_group(k, k), axis=1, keepdims=True)
        val_all = by_group(val, val)
        q_bf = q_all.astype(BF16)
        pos_all = by_group(pos, pos).astype(jnp.int32)
        for cp in kv_copies(c):
            cp.wait()

        def cached(i, g):
            return big[ff + 8 * ctx * g:ff + 8 * ctx * (g + 1), (2 * c + i) * head:(2 * c + i + 1) * head]

        for g in range(groups):
            sbuf[16 * g:16 * g + 16, :] = lax.dot_general(q_bf[16 * g:16 * g + 16], cached(0, g), (((1,), (1,)), ((), ())), preferred_element_type=F32)
        lane = lax.broadcasted_iota(jnp.int32, (2 * rows, 8 * ctx), 1)
        row = lax.broadcasted_iota(jnp.int32, (2 * rows, 8 * ctx), 0)
        valid = jnp.logical_and(lane // ctx == row % 8, lane % ctx < pos_all)
        s = ATTN_CAP * jnp.tanh(sbuf[:2 * rows, :] * (score_scale / ATTN_CAP))
        s_new = ATTN_CAP * jnp.tanh(s_new * (score_scale / ATTN_CAP))
        s = jnp.where(valid, s, -1e30)
        top = jnp.maximum(jnp.max(s, axis=1, keepdims=True), s_new)
        p = jnp.where(valid, jnp.exp(s - top), 0.0)
        p_new = jnp.exp(s_new - top)
        denom = jnp.sum(p, axis=1, keepdims=True) + p_new
        p_bf = p.astype(BF16)
        for g in range(groups):
            sbuf[16 * g:16 * g + 16, :head] = jnp.dot(p_bf[16 * g:16 * g + 16], cached(1, g), preferred_element_type=F32)
        o_all = (sbuf[:2 * rows, :head] + p_new.astype(BF16).astype(F32) * val_all) / denom
        o0 = jnp.concatenate([o_all[16 * g:16 * g + 8] for g in range(groups)], axis=0)
        o1 = jnp.concatenate([o_all[16 * g + 8:16 * g + 16] for g in range(groups)], axis=0)
        if c == 0:
            w_copies[3].wait()
        o = jnp.concatenate([o0, o1], axis=1).astype(BF16)
        part[c, :rows, :] = jnp.dot(o, wo[...], preferred_element_type=F32)
        if c + 1 == chunks:
            for cp in w_copies[4:]:
                cp.start()

    order = ((2, 1), (1, 2))

    def cols(h):
        return pl.ds(h * half, half)

    def rows_of(c, o):
        return pl.ds(pl.multiple_of(o * PIECES[c], 8), PIECES[c])

    def y_rows(c, o):
        return pl.ds(pl.multiple_of(group_rows(c) + o * PIECES[c], 8), PIECES[c])

    def remote(src, dst, c, phase, h, i, mask):
        return pltpu.make_async_remote_copy(src_ref=src, dst_ref=dst, send_sem=send_sem.at[c, phase, h, i], recv_sem=recv_sem.at[c, phase, h, i],
                                            device_id=(flip_t(t, mask), v), device_id_type=MESH)

    def scatter1(c, phase, h, i):
        m1, m2 = order[h]
        owner = flip_t(t, 3) if i else flip_t(t, m1)
        return remote(part.at[c, rows_of(c, owner), cols(h)], red1.at[c, h, i, pl.ds(0, PIECES[c])], c, phase, h, i, m1)

    def scatter2(c, phase, h):
        return remote(red1.at[c, h, 1, pl.ds(0, PIECES[c])], red2.at[c, h, pl.ds(0, PIECES[c])], c, phase, h, 2, order[h][1])

    def scatter_start(c, phase, halves=(0, 1)):
        for i in (1, 0):
            for h in halves:
                scatter1(c, phase, h, i).start()

    def scatter_pass(c, phase):
        n = PIECES[c]
        for h in range(2):
            scatter1(c, phase, h, 1).wait_recv()
            red1[c, h, 1, :n] = red1[c, h, 1, :n] + part[c, rows_of(c, flip_t(t, order[h][1])), h * half:(h + 1) * half]
            scatter2(c, phase, h).start()

    def scatter_end(c, phase):
        n = PIECES[c]
        got = []
        for h in range(2):
            scatter1(c, phase, h, 0).wait_recv()
            scatter2(c, phase, h).wait_recv()
            got.append(part[c, rows_of(c, t), h * half:(h + 1) * half] + red1[c, h, 0, :n] + red2[c, h, :n])
        for h in range(2):
            scatter1(c, phase, h, 0).wait_send()
            scatter1(c, phase, h, 1).wait_send()
            scatter2(c, phase, h).wait_send()
        return jnp.concatenate(got, axis=1)

    def gather(c, h, i):
        m1, m2 = order[h]
        where = ybuf.at[y_rows(c, flip_t(t, m2) if i == 2 else t), cols(h)]
        return remote(where, where, c, 1, h, i, m1 if i else m2)

    def gather_start(c):
        for i in (0, 1):
            for h in range(2):
                gather(c, h, i).start()

    def gather_pass(c):
        for h in range(2):
            gather(c, h, 0).wait_recv()
            gather(c, h, 2).start()

    def gather_end(c):
        for h in range(2):
            gather(c, h, 1).wait_recv()
            gather(c, h, 2).wait_recv()
        for h in range(2):
            for i in range(3):
                gather(c, h, i).wait_send()

    def middle(c):
        attn_out = scatter_end(c, 0)
        x_own = xbuf[c, rows_of(c, t), :].astype(F32)
        x1 = (x_own + rms(attn_out, gain(g_attn_post))).astype(BF16).astype(F32)
        mid[c, :PIECES[c]] = x1
        ybuf[y_rows(c, t), :] = rms(x1, gain(g_mlp_pre)).astype(BF16).astype(F32)

    def mlp(c, send):
        rows = groups_of[c]
        gather_end(c)
        if c == 0:
            for cp in w_copies[4:]:
                cp.wait()
        m = ybuf[pl.ds(group_rows(c), rows), :].astype(BF16)
        tiles = 3
        wide = ff // tiles

        def up_tile(i, carry):
            at = pl.ds(pl.multiple_of(i * wide, 128), wide)
            gate = jnp.dot(m, big[:width, at], preferred_element_type=F32)
            up = jnp.dot(m, big[width:2 * width, at], preferred_element_type=F32)
            act[:rows, at] = (jax.nn.gelu(gate, approximate=True) * up).astype(BF16)
            return carry

        lax.fori_loop(0, tiles, up_tile, 0)

        for h in range(2):
            part[c, :rows, h * half:(h + 1) * half] = jnp.dot(act[:rows, :], big[2 * width:2 * width + ff, h * half:(h + 1) * half], preferred_element_type=F32)
            if send:
                scatter_start(c, 2, (h,))

    def finish(c):
        y = (mid[c, :PIECES[c]] + rms(scatter_end(c, 2), gain(g_mlp_post))).astype(BF16).astype(F32)
        ybuf[y_rows(c, t), :] = y
        spread(c, 0)

    def axes_of(p, bits):
        axes = [AXES[(p + s) % 3] for s in range(3)]
        mt = mv = 0
        for s in range(3):
            if bits >> s & 1:
                mt ^= FLIP[axes[s]][0]
                mv ^= FLIP[axes[s]][1]
        return mt, mv

    def block_copy(c, p, s, bits):
        mt, mv = axes_of(p, bits)
        blk = 4 * flip_v(v, mv) + flip_t(t, mt)
        at = ybuf.at[pl.ds(pl.multiple_of(bases[c] + blk * PIECES[c], 8), PIECES[c]), pl.ds(p * third, third)]
        ft, fv = FLIP['c'] if s == 3 else FLIP[AXES[(p + s) % 3]]
        i = 2 ** s - 1 + bits
        return pltpu.make_async_remote_copy(src_ref=at, dst_ref=at, send_sem=spread_send.at[c, p, i], recv_sem=spread_recv.at[c, p, i],
                                            device_id=(flip_t(t, ft), flip_v(v, fv)), device_id_type=MESH)

    def spread(c, step):
        if step == 0:
            for s in (0, 1, 2, 3):
                for p in range(3):
                    block_copy(c, p, s, 0).start()
        elif step <= 3:
            s = step - 1
            for bits in range(2 ** s):
                for p in range(3):
                    block_copy(c, p, s, bits).wait_recv()
                    for later in range(s + 1, 4):
                        block_copy(c, p, later, bits | 1 << s).start()
        else:
            for p in range(3):
                for bits in range(8):
                    block_copy(c, p, 3, bits).wait_recv()

    def spread_sent(c):
        for p in range(3):
            for s in range(4):
                for bits in range(2 ** s):
                    block_copy(c, p, s, bits).wait_send()

    sub = E_ROWS // 4
    vocab_local = e_hbm.shape[0]
    tiles = vocab_local // E_ROWS
    total = tiles * chunks

    def e_copy(i):
        return pltpu.make_async_copy(e_hbm.at[pl.ds(pl.multiple_of(i % tiles * E_ROWS, E_ROWS), E_ROWS)],
                                     big.at[pl.ds(pl.multiple_of(i % E_SLOTS * E_ROWS, E_ROWS), E_ROWS)], e_sem.at[i % E_SLOTS])

    def y_copy(c):
        return pltpu.make_async_copy(wo.at[pl.ds(0, toks_of[c])], y_hbm.at[pl.ds(bases[c], toks_of[c])], y_sem.at[c])

    def stat_copy(c, j):
        other = (me + j) % 16
        return pltpu.make_async_remote_copy(src_ref=stat.at[c], dst_ref=stats.at[c, me], send_sem=stat_send.at[c, j - 1], recv_sem=stat_recv.at[c, j - 1],
                                            device_id=(other % 4, other // 4), device_id_type=MESH)

    def reduce_rows(lg, toks, tgt, first_row):
        rel = tgt - first_row
        sublane = lax.broadcasted_iota(jnp.int32, (8, toks), 0)
        s_acc = [jnp.zeros((8, toks), F32) for _ in range(2)]
        t_acc = [jnp.zeros((8, toks), F32) for _ in range(2)]
        for r in range(sub // 8):
            th = jnp.tanh(lg[8 * r:8 * r + 8, :toks] * (1.0 / FINAL_CAP))
            s_acc[r % 2] = s_acc[r % 2] + jnp.exp(th * FINAL_CAP)
            t_acc[r % 2] = t_acc[r % 2] + jnp.where(sublane == rel - 8 * r, th, 0.0)
        return s_acc[0] + s_acc[1], t_acc[0] + t_acc[1]

    def head_pass(c, per, tasks):
        toks = toks_of[c]
        strip = 128
        if c:
            y_copy(c - 1).wait()
        for r in range(toks // strip):
            yv = ybuf[bases[c] + r * strip:bases[c] + (r + 1) * strip, :]
            wo[r * strip:(r + 1) * strip, :] = yv.astype(BF16)
            wq[:, r * strip:(r + 1) * strip] = rms(yv, gain(g_final)).astype(BF16).T
        y_copy(c).start()
        first = bases[c] // 128
        tgt = jnp.concatenate([tgt_ref[first + q:first + q + 1, :] for q in range(toks // 128)], axis=1)
        tgt = jnp.broadcast_to(tgt, (8, toks)) - me * vocab_local

        def step(i, carry):
            s_sum, t_sum = carry
            n = c * tiles + i * per
            for k in range(per):
                e_copy(n + k).wait()
            for j in range(4 * per):
                now, before = (lg0, lg1) if j % 2 == 0 else (lg1, lg0)
                at = (n + j // 4) % E_SLOTS * E_ROWS + j % 4 * sub
                now[:, :toks] = jnp.dot(big[pl.ds(pl.multiple_of(at, sub), sub), :], wq[:, :toks], preferred_element_type=F32)
                s_part, t_part = reduce_rows(before, toks, tgt, i * per * E_ROWS + (j - 1) * sub)
                if j == 0:
                    s_part, t_part = jnp.where(i > 0, s_part, 0.0), jnp.where(i > 0, t_part, 0.0)
                s_sum, t_sum = s_sum + s_part, t_sum + t_part

            for k in range(per):
                @pl.when(n + k + E_SLOTS < total)
                def _(k=k):
                    e_copy(n + k + E_SLOTS).start()

            for at, task in tasks:
                @pl.when(i == at)
                def _(task=task):
                    task()

            return s_sum, t_sum

        zero = jnp.zeros((8, toks), F32)
        s_sum, t_sum = lax.fori_loop(0, tiles // per, step, (zero, zero))
        s_part, t_part = reduce_rows(lg1, toks, tgt, tiles * E_ROWS - sub)
        s_sum = jnp.sum(s_sum + s_part, axis=0, keepdims=True)
        t_sum = jnp.sum(t_sum + t_part, axis=0, keepdims=True)
        rows8 = [z[:, 128 * q:128 * (q + 1)] for z in (s_sum, t_sum) for q in range(toks // 128)]
        both = jnp.concatenate(rows8, axis=0)
        stat[c] = both
        stats[c, me] = both
        for j in range(1, 16):
            stat_copy(c, j).start()

    attend(0)
    lg1[...] = jnp.zeros_like(lg1)
    pl.semaphore_wait(barrier, 15)
    scatter_start(0, 0)
    attend(1)
    scatter_pass(0, 0)
    scatter_start(1, 0)
    middle(0)
    gather_start(0)
    scatter_pass(1, 0)
    gather_pass(0)
    middle(1)
    gather_start(1)
    mlp(0, True)
    scatter_pass(0, 2)
    gather_pass(1)
    finish(0)
    spread(0, 1)
    mlp(1, False)
    for i in range(E_SLOTS):
        e_copy(i).start()
    spread(0, 2)
    spread(0, 3)
    spread(0, 4)
    scatter_start(1, 2)
    head_pass(0, 1, ((0, lambda: scatter_pass(1, 2)), (2, lambda: finish(1)), (3, lambda: spread(1, 1)), (5, lambda: spread(1, 2)), (7, lambda: spread(1, 3)), (9, lambda: spread(1, 4))))
    head_pass(1, 2, ())
    for c in range(chunks):
        spread_sent(c)
        for j in range(1, 16):
            stat_copy(c, j).wait_recv()
            stat_copy(c, j).wait_send()
    y_copy(chunks - 1).wait()


def out_kernel(stats_hbm, y_hbm, logp_hbm, out_hbm, stats, logp, ybuf, stat_sem, in_sem, out_sem):
    pieces = in_sem.shape[0]
    n = ybuf.shape[0] // pieces
    get = pltpu.make_async_copy(stats_hbm, stats, stat_sem.at[0])
    get.start()

    def y_in(i):
        return pltpu.make_async_copy(y_hbm.at[pl.ds(i * n, n)], ybuf.at[pl.ds(i * n, n)], in_sem.at[i])

    def y_out(i):
        return pltpu.make_async_copy(ybuf.at[pl.ds(i * n, n)], out_hbm.at[pl.ds(i * n, n)], out_sem.at[i])

    for i in range(pieces):
        y_in(i).start()
    get.wait()
    first = 0
    for c, piece in enumerate(PIECES):
        tot = stats[c, 0]
        for b in range(1, stats.shape[1]):
            tot = tot + stats[c, b]
        rows = piece * 16 // 128
        logp[first:first + rows, :] = FINAL_CAP * tot[rows:2 * rows] - jnp.log(tot[:rows])
        first += rows
    put = pltpu.make_async_copy(logp, logp_hbm, stat_sem.at[1])
    put.start()
    for i in range(pieces):
        y_in(i).wait()
        y_out(i).start()
    put.wait()
    for i in range(pieces):
        y_out(i).wait()


def collect(stats, y):
    hbm = pl.BlockSpec(memory_space=pl.ANY)
    dma = pltpu.SemaphoreType.DMA
    return pl.pallas_call(
        out_kernel,
        out_shape=(jax.ShapeDtypeStruct((y.shape[0] // 128, 128), F32), jax.ShapeDtypeStruct(y.shape, y.dtype)),
        in_specs=[hbm, hbm],
        out_specs=(hbm, hbm),
        scratch_shapes=[pltpu.VMEM(stats.shape, F32), pltpu.VMEM((y.shape[0] // 128, 128), F32), pltpu.VMEM(y.shape, y.dtype), dma((2,)), dma((8,)), dma((8,))],
        name='collect',
    )(stats, y)


def step_kernel(x, seq, tgt, freq, gains, w_q, w_k, w_v, w_o, w_gate, w_up, w_down, k_rows, v_rows, table):
    tokens, width = x.shape
    chunks = len(PIECES)
    top = max(PIECES)
    rows, toks = 4 * top, 16 * top
    head = w_k.shape[1]
    ctx = k_rows.shape[0] // tokens
    ff = w_gate.shape[1]
    vm = pl.BlockSpec(memory_space=pltpu.VMEM)
    hbm = pl.BlockSpec(memory_space=pl.ANY)
    dma = pltpu.SemaphoreType.DMA
    return pl.pallas_call(
        kernel,
        out_shape=(jax.ShapeDtypeStruct((chunks, 16, 8, 128), F32), jax.ShapeDtypeStruct((tokens, width), BF16)),
        in_specs=[hbm] + [vm] * 8 + [hbm] * 10,
        out_specs=(vm, hbm),
        scratch_shapes=[
            pltpu.VMEM((chunks, rows, width), BF16),
            pltpu.VMEM(w_q.shape, BF16),
            pltpu.VMEM(w_k.shape, BF16),
            pltpu.VMEM(w_v.shape, BF16),
            pltpu.VMEM(w_o.shape, BF16),
            pltpu.VMEM((2 * width + ff, ff), BF16),
            pltpu.VMEM((2 * rows, 8 * ctx), F32),
            pltpu.VMEM((chunks, rows, width), F32),
            pltpu.VMEM((chunks, 2, 2, top, width // 2), F32),
            pltpu.VMEM((chunks, 2, top, width // 2), F32),
            pltpu.VMEM((tokens, width), F32),
            pltpu.VMEM((chunks, top, width), F32),
            pltpu.VMEM((rows, ff), BF16),
            pltpu.VMEM((E_ROWS // 4, toks), F32),
            pltpu.VMEM((E_ROWS // 4, toks), F32),
            pltpu.VMEM((chunks, 8, 128), F32),
            dma((chunks,)),
            dma((7,)),
            dma((chunks, 2)),
            dma((E_SLOTS,)),
            dma((chunks,)),
            dma((chunks, 3, 2, 3)),
            dma((chunks, 3, 2, 3)),
            dma((chunks, 3, 15)),
            dma((chunks, 3, 15)),
            dma((chunks, 15)),
            dma((chunks, 15)),
        ],
        compiler_params=pltpu.CompilerParams(collective_id=0, has_side_effects=True, vmem_limit_bytes=67_000_000),
        name='step',
    )(x, seq, tgt, freq, *gains, w_q, w_k, w_v, w_o, w_gate, w_up, w_down, k_rows, v_rows, table)


def solution(mesh):
    in_specs = (P(), P(), P(), P(), P(None, 't'), P(None, 't'), P(None, 't'), P('t', None), P(), P(), P(None, 't'), P(None, 't'), P('t', None), P(), P(), P(None, None, 't', None), P(None, None, 't', None), P(('v', 't'), None))

    def local_step(hidden_in, seq_lens, target, g_attn_pre, w_q, w_k, w_v, w_o, g_attn_post, g_mlp_pre, w_gate, w_up, w_down, g_mlp_post, g_final, k_cache, v_cache, embed_table):
        tokens = hidden_in.shape[0]
        ctx, _, head_dim = k_cache.shape[1:]
        freq = ROPE_BASE ** (-2.0 * np.arange(head_dim // 2, dtype=np.float32) / head_dim)
        stats, y = step_kernel(
            hidden_in, seq_lens.reshape(-1, 128), target.reshape(-1, 128), jnp.asarray(freq[None, :], F32),
            (g_attn_pre, g_attn_post, g_mlp_pre, g_mlp_post, g_final), w_q, w_k, w_v, w_o, w_gate, w_up, w_down,
            k_cache.reshape(tokens * ctx, head_dim), v_cache.reshape(tokens * ctx, head_dim), embed_table)
        logp, hidden_out = collect(stats, y)
        return logp.reshape(tokens), hidden_out

    return jax.shard_map(local_step, mesh=mesh, in_specs=in_specs, out_specs=(P(), P()), check_vma=False)
```
